256 devices in a mesh: view: 8 (over x, core), gauss: 32 (over y, z).
Axes of the slice: x: 4, y: 4, z: 8, core: 2. Of those that a mesh axis runs over, the one named last changes fastest.
Arguments:
- means: float32 [3, 524288], P(None, 'gauss'), may hold values from -1 to 1
- scales: float32 [3, 524288], P(None, 'gauss'), may hold values from 0.05 to 0.6
- quats: float32 [4, 524288], P(None, 'gauss'), may hold values from -6 to 6
- attrs: float32 [49, 524288], P(None, 'gauss'), may hold values from -6 to 6
- grad_screen: float32 [32, 2, 524288], P('view', None, 'gauss'), may hold values from -6 to 6
- visible: int32 [32, 524288], P('view', 'gauss'), may hold values 0 or 1
- clone_mask: int32 [524288], P('gauss'), may hold values from 0 to 1, as said below
- rotation: float32 [32, 3, 3], P('view'), may hold values from -3.5 to 3.5
- shift: float32 [32, 3], P('view'), may hold values from 2 to 5
- focal: float32 [32], P('view'), may hold values from 1 to 4
Outputs:
- peak_stats: float32 [2, 524288], P(None, 'gauss')
- clones: float32 [61, 524288], P(None, 'gauss')
- clone_total: int32 [], replicated
The draws below stay inside these ranges and needn't reach their ends.
Inputs may be any that keep to these rules, and one draw needn't show every extreme that they name: `clone_mask`: in every draw some shard of 16384 consecutive Gaussians has all of them marked.
All inputs are finite; a program needn't handle non-finite values. No bound on the sum of `visible` on one device may be relied on, other than what follows from the above.
Results may differ from the reference program's by a relative error of at most 0.0003.
Values sent between devices are 32-bit elements; how exact they have to be, the bound alone decides.
A program may use at most 128 MiB of HBM per device.

```python
import math
import jax
import jax.numpy as jnp
from jax import lax

G_DEV = 16384
ATTR = 49
GAUSSIANS = 524288
VIEWS = 32
N_GAUSS = 32


def draw_clone_mask(key, part):
    shards = GAUSSIANS // G_DEV
    most = G_DEV // 128 * 128
    first, second, third = jax.random.split(key, 3)
    raw = jax.random.randint(first, (shards,), 0, most + 1)
    counts = raw * raw // most
    chosen = jax.random.randint(second, (), 0, shards)
    counts = jnp.where(jnp.arange(shards) == chosen, most, counts)
    keys = jax.random.split(third, shards)
    orders = jax.vmap(lambda k: jax.random.permutation(k, G_DEV))(keys)
    return (orders < counts[:, None]).astype(jnp.int32).reshape(-1)


def with_ends(result, stream_key, least, high):
    longest = result.shape.index(max(result.shape))
    spots = []
    for shift in (0, 1):
        where = [jax.random.randint(jax.random.fold_in(stream_key, axis), (), 0, length) for axis, length in enumerate(result.shape)]
        where[longest] = (where[longest] + shift) % result.shape[longest]
        spots.append(tuple(where))
    return result.at[spots[0]].set(least).at[spots[1]].set(high)


def level_of(own_key, extent, pieces, smallest, top_value):
    def one(dim, shards_of):
        steps = jax.random.uniform(jax.random.fold_in(jax.random.fold_in(own_key, 6), dim), (shards_of,), jnp.float32, smallest / len(pieces), top_value / len(pieces))
        return jnp.repeat(jnp.exp(steps), extent[dim] // shards_of).reshape((-1,) + (1,) * (len(extent) - dim - 1))

    loudness = one(*pieces[0])
    for cut in pieces[1:]:
        loudness = loudness * one(*cut)
    return loudness


def centred(own_key, dims, deviation, reach, cuts=(), dtype=jnp.bfloat16):
    result = deviation * jax.random.normal(own_key, dims, jnp.float32)
    if cuts:
        result = result * level_of(own_key, dims, cuts, -0.22, 0.18)
    return jnp.clip(result, -reach, reach).astype(dtype)


def setup_inputs(seed: int = 0) -> dict:
    arg_keys = jax.random.split(jax.random.key(seed), 11)
    return {
        "means": jnp.clip(jax.random.uniform(arg_keys[0], (3, GAUSSIANS), jnp.float32, -1.0, 1.0) * level_of(arg_keys[0], (3, GAUSSIANS), ((1, 32),), -0.4, 0.0), -1.0, 1.0),
        "scales": jnp.clip(jnp.exp(math.log(0.6) - 2.4849067 * jax.random.uniform(arg_keys[1], (3, GAUSSIANS), jnp.float32) ** level_of(arg_keys[1], (3, GAUSSIANS), ((1, 32),), -0.2, 0.2)), 0.05, 0.6),
        "quats": centred(arg_keys[2], (4, GAUSSIANS), 1.0, 6.0, ((1, 32),), jnp.float32),
        "attrs": centred(arg_keys[3], (ATTR, GAUSSIANS), 1.0, 6.0, ((1, 32),), jnp.float32),
        "grad_screen": centred(arg_keys[4], (VIEWS, 2, GAUSSIANS), 1.0, 6.0, ((0, 8), (2, 32)), jnp.float32),
        "visible": with_ends((jax.random.randint(arg_keys[5], (VIEWS, GAUSSIANS), 0, 4) < 3).astype(jnp.int32), jax.random.fold_in(arg_keys[5], 1), 0, 1),
        "clone_mask": draw_clone_mask(jax.random.fold_in(arg_keys[10], 71), 0),
        "rotation": centred(arg_keys[7], (VIEWS, 3, 3), 3 ** -0.5, 3.5, ((0, 8),), jnp.float32),
        "shift": jnp.clip(2.0 + 3.0 * jax.random.uniform(arg_keys[8], (VIEWS, 3), jnp.float32) ** level_of(arg_keys[8], (VIEWS, 3), ((0, 8),), -0.2, 0.2), 2.0, 5.0),
        "focal": jnp.clip(jnp.exp(math.log(4.0) - 1.3862944 * jax.random.uniform(arg_keys[9], (VIEWS,), jnp.float32) ** level_of(arg_keys[9], (VIEWS,), ((0, 8),), -0.2, 0.2)), 1.0, 4.0),
    }


def quat_factor(scales, quats):
    inv = 1.0 / jnp.sqrt(lax.optimization_barrier(jnp.sum(quats * quats, axis=0)) + 0.25)
    w, x, y, z = (quats[0] * inv, quats[1] * inv, quats[2] * inv, quats[3] * inv)
    rq = [[1 - 2 * (y * y + z * z), 2 * (x * y - w * z), 2 * (x * z + w * y)], [2 * (x * y + w * z), 1 - 2 * (x * x + z * z), 2 * (y * z - w * x)], [2 * (x * z - w * y), 2 * (y * z + w * x), 1 - 2 * (x * x + y * y)]]
    return [[rq[i][j] * scales[j] for j in range(3)] for i in range(3)]

def view_stats(means, factor, grad, seen, rot, trans, focal_v):
    point = [rot[i, 0] * means[0] + rot[i, 1] * means[1] + rot[i, 2] * means[2] + trans[i] for i in range(3)]
    depth = jnp.maximum(point[2], 1.0)
    j00 = focal_v / depth
    j02 = -focal_v * point[0] / (depth * depth)
    j12 = -focal_v * point[1] / (depth * depth)
    first = [j00 * rot[0, j] + j02 * rot[2, j] for j in range(3)]
    second = [j00 * rot[1, j] + j12 * rot[2, j] for j in range(3)]
    prow = [sum((first[j] * factor[j][k] for j in range(3))) for k in range(3)]
    qrow = [sum((second[j] * factor[j][k] for j in range(3))) for k in range(3)]
    a_val = prow[0] ** 2 + prow[1] ** 2 + prow[2] ** 2 + 0.3
    c_val = qrow[0] ** 2 + qrow[1] ** 2 + qrow[2] ** 2 + 0.3
    b_val = prow[0] * qrow[0] + prow[1] * qrow[1] + prow[2] * qrow[2]
    half = 0.5 * (a_val - c_val)
    lam = 0.5 * (a_val + c_val) + jnp.sqrt(half * half + b_val * b_val + 0.01)
    seenf = seen.astype(jnp.float32)
    radius = 3.0 * jnp.sqrt(lam) * seenf
    gnorm = jnp.sqrt(grad[0] * grad[0] + grad[1] * grad[1]) * seenf
    return (gnorm, radius)

def reference(means, scales, quats, attrs, grad_screen, visible, clone_mask, rotation, shift, focal):
    factor = quat_factor(scales, quats)
    gmax = jnp.zeros(means.shape[1], jnp.float32)
    rmax = jnp.zeros(means.shape[1], jnp.float32)
    for v in range(grad_screen.shape[0]):
        gnorm, radius = view_stats(means, factor, grad_screen[v], visible[v], rotation[v], shift[v], focal[v])
        gmax = jnp.maximum(gmax, gnorm)
        rmax = jnp.maximum(rmax, radius)
    peak = jnp.stack([gmax, rmax])
    rows = jnp.concatenate([means, scales, quats, attrs, peak], axis=0)
    shards = N_GAUSS
    cap = G_DEV // 128 * 128
    marks = clone_mask.reshape(shards, G_DEV)
    rank = jnp.cumsum(marks, axis=1).astype(jnp.int32) - 1
    counts = lax.optimization_barrier(jnp.sum(marks, axis=1)).astype(jnp.int32)
    blocks = (counts + 127) // 128
    offset = (jnp.cumsum(blocks) - blocks).astype(jnp.int32)
    block = offset[:, None] + rank // 128
    column = block % shards * cap + block // shards * 128 + rank % 128
    column = jnp.where(marks == 1, column, shards * cap).reshape(-1).astype(jnp.int32)
    clones = jnp.zeros((rows.shape[0], shards * cap), jnp.float32).at[:, column].set(rows, mode='drop')
    total = jnp.sum(clone_mask).astype(jnp.int32)
    return (peak, clones, total)
```

```python
import functools

import jax
import jax.numpy as jnp
from jax import lax
from jax.experimental import pallas as pl
from jax.experimental.pallas import tpu as pltpu
from jax.sharding import PartitionSpec as P

LANES = 128
SUB = 8
TILES = 8
VMEM = pltpu.VMEM
SMEM = pltpu.SMEM
HBM = pltpu.HBM
MESH = pl.DeviceIdType.MESH


def spec(space):
    return pl.BlockSpec(memory_space=space)


def peer(view, gauss):
    return {"view": view, "gauss": gauss}


def quat_factor(scales, quats):
    w, x, y, z = quats
    inv = 1.0 / jnp.sqrt(w * w + x * x + y * y + z * z + 0.25)
    w, x, y, z = (w * inv, x * inv, y * inv, z * inv)
    rq = [
        [1 - 2 * (y * y + z * z), 2 * (x * y - w * z), 2 * (x * z + w * y)],
        [2 * (x * y + w * z), 1 - 2 * (x * x + z * z), 2 * (y * z - w * x)],
        [2 * (x * z - w * y), 2 * (y * z + w * x), 1 - 2 * (x * x + y * y)],
    ]
    return [[rq[i][j] * scales[j] for j in range(3)] for i in range(3)]


def view_radius(means, factor, rot, trans, focal_v):
    point = [
        rot[i][0] * means[0] + rot[i][1] * means[1] + rot[i][2] * means[2] + trans[i]
        for i in range(3)
    ]
    inv = 1.0 / jnp.maximum(point[2], 1.0)
    j00 = focal_v * inv
    j02 = -(j00 * point[0]) * inv
    j12 = -(j00 * point[1]) * inv
    first = [j00 * rot[0][j] + j02 * rot[2][j] for j in range(3)]
    second = [j00 * rot[1][j] + j12 * rot[2][j] for j in range(3)]
    prow = [sum((first[j] * factor[j][k] for j in range(3))) for k in range(3)]
    qrow = [sum((second[j] * factor[j][k] for j in range(3))) for k in range(3)]
    a_val = prow[0] * prow[0] + prow[1] * prow[1] + prow[2] * prow[2] + 0.3
    c_val = qrow[0] * qrow[0] + qrow[1] * qrow[1] + qrow[2] * qrow[2] + 0.3
    b_val = prow[0] * qrow[0] + prow[1] * qrow[1] + prow[2] * qrow[2]
    half = 0.5 * (a_val - c_val)
    lam = 0.5 * (a_val + c_val) + jnp.sqrt(half * half + b_val * b_val + 0.01)
    return 3.0 * jnp.sqrt(lam)


YO = (0, 1, 3, 2)
ZO = (0, 1, 7, 2, 6, 3, 5, 4)
GROUPS = (4, 4, 8, 8, 8)


def pick(table, index):
    out = jnp.full(index.shape, table[0], jnp.int32)
    for i in range(1, len(table)):
        out = jnp.where(index == i, table[i], out)
    return out


def main_kernel(
    V, S, views, rots_h, trns_h, foc_h, mask_h, means_h, scales_h, quats_h, attrs_h, grad_h, vis_h,
    buf, peak, where_out,
    rots, trns, foc, mask, means, scales, quats, grad, vis, x, enc, g, split, send, cnt, counts,
    local, halves, merged, whole, lsem, csend, crecv, rsend, rrecv, asend, arecv,
    fsend, frecv, xsend, xrecv, hsend, hrecv, msend, mrecv,
):
    v, s = lax.axis_index("view"), lax.axis_index("gauss")
    nblk = mask.shape[0]
    per = nblk // S
    Z = len(ZO)
    Y = len(YO)
    X = V // 2
    core = lax.rem(v, 2)
    chip = lax.div(v, 2)
    mate = v + 1 - 2 * core
    nxt = 2 * lax.rem(chip + 1, X) + core
    prv = 2 * lax.rem(chip + X - 1, X) + core
    opp = 2 * lax.rem(chip + 2, X) + core
    y, z = lax.div(s, Z), lax.rem(s, Z)
    i32, f32, bf16 = jnp.int32, jnp.float32, jnp.bfloat16

    def dest(p):
        return lax.rem(y + YO[p // Z], Y) * Z + lax.rem(z + ZO[p % Z], Z)

    bar = pltpu.get_barrier_semaphore()
    for p in range(1, S):
        pl.semaphore_signal(bar, inc=1, device_id=peer(v, dest(p)), device_id_type=MESH)
    for k in range(1, V):
        pl.semaphore_signal(bar, inc=1, device_id=peer(lax.rem(v + k, V), s), device_id_type=MESH)

    loads = [
        pltpu.make_async_copy(a, b, lsem.at[i])
        for i, (a, b) in enumerate((
            (mask_h, mask), (means_h, means), (scales_h, scales), (quats_h, quats),
            (grad_h, grad), (vis_h, vis), (rots_h, rots), (trns_h, trns), (foc_h, foc),
        ))
    ]
    for c in loads:
        c.start()

    def tiles(act):
        for t in range(1, TILES):
            @pl.when(v == t)
            def _():
                n = 6 if t < TILES - 1 else 1
                act(pltpu.make_async_copy(
                    attrs_h.at[pl.ds((t - 1) * SUB, n), :], x.at[pl.ds(0, n), :], lsem.at[9]
                ))
                if t > 1:
                    act(pltpu.make_async_copy(
                        attrs_h.at[pl.ds((t - 2) * SUB + 6, 2), :], x.at[pl.ds(6, 2), :], lsem.at[10]
                    ))

    tiles(lambda c: c.start())

    loads[0].wait()
    m = mask[...]
    cnt[...] = jnp.full((1, LANES), jnp.sum(m), i32)
    lane = lax.broadcasted_iota(i32, (nblk, LANES), 1)
    row = lax.broadcasted_iota(i32, (nblk, LANES), 0)
    mb = m.astype(bf16)
    before = (row < lane).astype(bf16)
    above = (row > lane).astype(bf16)
    dot = functools.partial(jnp.dot, preferred_element_type=f32)
    ones = jnp.ones((LANES, LANES), bf16)
    rank = dot(mb, before).astype(i32)
    size = dot(mb, ones).astype(i32)
    base = dot(dot(above, mb).astype(bf16), ones).astype(i32)
    flat = lax.dot_general(
        jnp.ones((SUB, LANES), bf16), mb, (((1,), (1,)), ((), ())), preferred_element_type=f32
    )
    starts = dot(flat.astype(bf16), before).astype(i32)
    code = jnp.where(m == 1, 65536 + (lane - rank) * 256 + lane, 0)
    bit = 1
    while bit < LANES:
        moved = pltpu.roll(code, LANES - bit, 1)
        goes = (moved & (bit * 256)) != 0
        stays = (code & (bit * 256)) == 0
        code = jnp.where(goes, moved, jnp.where(stays, code, 0))
        bit *= 2
    turn = (lane - base) & (LANES - 1)
    src = jnp.take_along_axis(code & (LANES - 1), turn, axis=1)
    valid = turn < size
    idx = jnp.where(valid, src, 0)
    enc[...] = jnp.where(valid, src, -1)
    head = lane >= (base & (LANES - 1))
    low, high = valid & head, valid & jnp.logical_not(head)

    for c in loads[1:]:
        c.wait()
    step = 2 * SUB

    def chunk(i, carry):
        rows = pl.ds(pl.multiple_of(i * step, step), step)

        def lines(ref, count, c):
            return ref[pl.ds(i * step * count + c, step, stride=count), :]

        mm = [means[rows, c, :] for c in range(3)]
        factor = quat_factor(
            [scales[rows, c, :] for c in range(3)], [lines(quats, 4, c) for c in range(4)]
        )
        gmax = jnp.zeros((step, LANES), f32)
        rmax = jnp.zeros((step, LANES), f32)
        for u in range(views):
            rot = [[rots[a, u, b] for b in range(3)] for a in range(3)]
            trans = [trns[u, a] for a in range(3)]
            radius = view_radius(mm, factor, rot, trans, foc[u])
            seen = lines(vis, views, u).astype(f32)
            g0, g1 = (grad[u, pl.ds(i * step * 2 + c, step, stride=2), :] for c in range(2))
            gmax = jnp.maximum(gmax, jnp.sqrt(g0 * g0 + g1 * g1) * seen)
            rmax = jnp.maximum(rmax, radius * seen)
        local[pl.ds(i * step * 2, step, stride=2), :] = gmax
        local[pl.ds(i * step * 2 + 1, step, stride=2), :] = rmax
        return carry

    lax.fori_loop(0, nblk // step, chunk, 0)

    started = []

    def remote(a, b, ss, rs, to):
        return pltpu.make_async_remote_copy(
            src_ref=a, dst_ref=b, send_sem=ss, recv_sem=rs, device_id=to, device_id_type=MESH
        )

    def go(copy):
        copy.start()
        started.append(copy)
        return copy

    pl.semaphore_wait(bar, S + V - 2)
    tally = [
        go(remote(cnt, counts.at[pl.ds(p, 1), :], csend.at[p], crecv.at[p], peer(v, dest(p))))
        for p in range(1, S)
    ]
    piece = 2 * nblk // V
    scatter = []
    for k in range(1, V):
        to = lax.rem(v + k, V)
        part = local.at[pl.ds(pl.multiple_of(to * piece, piece), piece), :]
        scatter.append(go(remote(part, halves.at[k], rsend.at[k], rrecv.at[k], peer(to, s))))
    counts[0:1, :] = cnt[...]

    tiles(lambda c: c.wait())

    @pl.when(v > 0)
    def _():
        def gather(b, carry):
            e = jnp.broadcast_to(enc[pl.ds(b, 1), :], (SUB, LANES))
            cols = pl.ds(pl.multiple_of(b * LANES, LANES), LANES)
            got = jnp.take_along_axis(x[:, cols], jnp.maximum(e, 0), axis=1)
            g[b] = got
            return carry

        lax.fori_loop(0, nblk, gather, 0, unroll=8)

    def put(final, value):
        g[:, (final + 6) % SUB, :] = jnp.take_along_axis(value, idx, axis=1)

    @pl.when(v == 0)
    def _():
        for c in range(3):
            put(c, means[:, c, :])
            put(3 + c, scales[:, c, :])
        for c in range(2):
            put(6 + c, quats[pl.ds(c, nblk, stride=4), :])

    @pl.when(v == 1)
    def _():
        for c in range(2):
            put(c, quats[pl.ds(2 + c, nblk, stride=4), :])

    def cut(c):
        value = g[:, (c + 6) % SUB, :]
        for part, keep in enumerate((low, high)):
            rest = jnp.where(keep, value, 0.0)
            for i in range(3):
                top = rest.astype(bf16)
                split[(2 * i + part) * nblk:(2 * i + part + 1) * nblk, c * LANES:(c + 1) * LANES] = top
                rest = rest - top.astype(f32)

    for c in range(3):
        cut(c)

    @pl.when(v < TILES - 1)
    def _():
        for c in range(3, SUB):
            cut(c)

    for c in scatter:
        c.wait_recv()
    mine = pl.ds(pl.multiple_of(v * piece, piece), piece)
    best = local[mine, :]
    for k in range(1, V):
        best = jnp.maximum(best, halves[k])
    merged[...] = best
    spread = [
        go(remote(merged, whole.at[k], asend.at[k], arecv.at[k], peer(lax.rem(v + k, V), s)))
        for k in range(1, V)
    ]
    peak[mine, :] = best
    for k in range(1, V):
        spread[k - 1].wait_recv()
        who = lax.rem(v + V - k, V)
        peak[pl.ds(pl.multiple_of(who * piece, piece), piece), :] = whole[k]

    @pl.when(v == TILES - 1)
    def _():
        for c in range(2):
            put(3 + c, peak[pl.ds(c, nblk, stride=2), :])
        for c in range(5, SUB):
            g[:, (c + 6) % SUB, :] = jnp.zeros((nblk, LANES), f32)
        for c in range(3, SUB):
            cut(c)

    for c in tally:
        c.wait_recv()
    tot = counts[...]
    blocks = (tot + (LANES - 1)) >> 7

    def source(p):
        return ((y - pick(YO, p >> 3)) & (Y - 1)) * Z + ((z - pick(ZO, p & 7)) & (Z - 1))

    pr = lax.broadcasted_iota(i32, (S, S), 0)
    pc = lax.broadcasted_iota(i32, (S, S), 1)
    less = (source(pc) < source(pr)).astype(bf16)
    offs = dot(less, blocks.astype(bf16)).astype(i32)
    t = ((y + pick(YO, row >> 5)) & (Y - 1)) * Z + ((z + pick(ZO, (row >> 2) & 7)) & (Z - 1))
    d = ((t - offs[0:1, :]) & (S - 1)) + ((row & (per - 1)) << 5)
    at = starts[0:1, :] >> 7
    a_low = (d == at).astype(bf16)
    a_high = (d == at + 1).astype(bf16)
    hot = jnp.concatenate([a_low, a_high] * 3, axis=1)
    moved = dot(hot, split[...])
    for c in range(SUB):
        send[:, c, :] = moved[:, c * LANES:(c + 1) * LANES]

    k = lax.broadcasted_iota(i32, (S, LANES), 1) * S + s
    p32 = lax.broadcasted_iota(i32, (S, LANES), 0)
    here = (k >= offs) & (k < offs + blocks)
    spot = jnp.where(here, p32 * per + ((k - offs) >> 5) + 1, 0)
    found = jnp.sum(spot, axis=0, keepdims=True) - 1
    total = jnp.sum(tot, axis=0, keepdims=True)
    sub = lax.broadcasted_iota(i32, (SUB, LANES), 0)
    where_out[...] = jnp.where(sub == 0, found, total)

    fars = [None]
    for p in range(1, S):
        fars.append(go(remote(
            send.at[pl.ds(p * per, per)], buf.at[v, pl.ds(p * per, per)],
            fsend.at[p], frecv.at[p], peer(v, dest(p)),
        )))
    own = pltpu.make_async_copy(send.at[pl.ds(0, per)], buf.at[v, pl.ds(0, per)], fsend.at[0])
    own.start()

    edges = [0]
    for n in GROUPS:
        edges.append(edges[-1] + n)
    N = len(GROUPS)

    def group(owner, i, half=None):
        first, size = edges[i] * per, GROUPS[i] * per
        if half is not None:
            size //= 2
            first += half * size
        return buf.at[owner, pl.ds(first, size)]

    def ring(i, way):
        return remote(group(v, i), group(v, i), xsend.at[way, i], xrecv.at[way, i], peer((nxt, prv)[way], s))

    def relay(i, way):
        ref = group((prv, nxt)[way], i, way)
        return remote(ref, ref, hsend.at[way, i], hrecv.at[way, i], peer((nxt, prv)[way], s))

    def beside(i, q):
        ref = group((v, prv, nxt, opp)[q], i)
        return remote(ref, ref, msend.at[q, i], mrecv.at[q, i], peer(mate, s))

    rings, relays, besides = {}, {}, {}
    for i in range(N + 2):
        if i < N:
            for p in range(edges[i], edges[i + 1]):
                if p:
                    fars[p].wait_recv()
                else:
                    own.wait()
            for way in range(2):
                rings[i, way] = go(ring(i, way))
            besides[i, 0] = go(beside(i, 0))
        if 1 <= i <= N:
            for way in range(2):
                rings[i - 1, way].wait_recv()
                relays[i - 1, way] = go(relay(i - 1, way))
                besides[i - 1, 1 + way] = go(beside(i - 1, 1 + way))
        if i >= 2:
            for way in range(2):
                relays[i - 2, way].wait_recv()
            besides[i - 2, 3] = go(beside(i - 2, 3))
    for c in besides.values():
        c.wait_recv()
    for c in started:
        c.wait_send()


def place_kernel(idx_v, peak_in, buf, clones, peak, total, out, idx, isem, osem, psem):
    rows = clones.shape[0]
    slots = out.shape[1] // LANES
    chunks = osem.shape[0]
    fetch = pltpu.make_async_copy(idx_v, idx, isem)
    fetch.start()
    top = pltpu.make_async_copy(peak_in, peak, psem)
    top.start()
    fetch.wait()
    total[0] = idx[1, 0]
    each = slots // chunks
    outs = []
    for c in range(chunks):
        def one(q, carry):
            r = idx[0, q]
            on = r >= 0
            r = jnp.maximum(r, 0)
            cols = pl.ds(pl.multiple_of(q * LANES, LANES), LANES)
            for i in range(TILES):
                n = min(rows - i * SUB, SUB)
                out[i * SUB:i * SUB + n, cols] = jnp.where(on, buf[i, r], 0.0)[:n]
            return carry

        lax.fori_loop(c * each, (c + 1) * each, one, 0, unroll=4)
        cols = pl.ds(c * each * LANES, each * LANES)
        cp = pltpu.make_async_copy(out.at[:, cols], clones.at[:, cols], osem.at[c])
        cp.start()
        outs.append(cp)
    for cp in outs:
        cp.wait()
    top.wait()


def body(V, S, means, scales, quats, attrs, grad_screen, visible, clone_mask, rotation, shift, focal):
    G = clone_mask.shape[0]
    nblk = G // LANES
    views = grad_screen.shape[0]
    rows = means.shape[0] + scales.shape[0] + quats.shape[0] + attrs.shape[0] + 2
    f32, i32 = jnp.float32, jnp.int32

    def lines(a):
        a = a.reshape(a.shape[:-1] + (nblk, LANES))
        return jnp.swapaxes(a, -3, -2)

    dma = pltpu.SemaphoreType.DMA
    piece = 2 * nblk // V
    N = len(GROUPS)
    limit = 32 * 1024 * 1024
    buf, peak, where = pl.pallas_call(
        functools.partial(main_kernel, V, S, views),
        out_shape=(
            VMEM((V, nblk, SUB, LANES), f32), VMEM((2 * nblk, LANES), f32), VMEM((SUB, LANES), i32),
        ),
        in_specs=[spec(HBM)] * 10,
        out_specs=(spec(VMEM),) * 3,
        scratch_shapes=[
            SMEM((3, views, 3), f32),
            SMEM((views, 3), f32),
            SMEM((views,), f32),
            VMEM((nblk, LANES), i32),
            VMEM((nblk, 3, LANES), f32),
            VMEM((nblk, 3, LANES), f32),
            VMEM((4 * nblk, LANES), f32),
            VMEM((views, 2 * nblk, LANES), f32),
            VMEM((views * nblk, LANES), i32),
            VMEM((SUB, G), f32),
            VMEM((nblk, LANES), i32),
            VMEM((nblk, SUB, LANES), f32),
            VMEM((6 * nblk, SUB * LANES), jnp.bfloat16),
            VMEM((nblk, SUB, LANES), f32),
            VMEM((1, LANES), i32),
            VMEM((S, LANES), i32),
            VMEM((2 * nblk, LANES), f32),
            VMEM((V, piece, LANES), f32),
            VMEM((piece, LANES), f32),
            VMEM((V, piece, LANES), f32),
            dma((11,)), dma((S,)), dma((S,)), dma((V,)), dma((V,)), dma((V,)), dma((V,)),
            dma((S,)), dma((S,)), dma((2, N)), dma((2, N)), dma((2, N)), dma((2, N)),
            dma((4, N)), dma((4, N)),
        ],
        compiler_params=pltpu.CompilerParams(
            collective_id=0, has_side_effects=True, vmem_limit_bytes=limit
        ),
        name="main",
    )(*(
        pltpu.with_memory_space_constraint(a, HBM)
        for a in (
            jnp.transpose(rotation, (1, 0, 2)), shift, focal, clone_mask.reshape(nblk, LANES),
            lines(means), lines(scales), lines(quats).reshape(-1, LANES), attrs,
            lines(grad_screen).reshape(views, -1, LANES), lines(visible).reshape(-1, LANES),
        )
    ))
    chunks = 8
    clones, peak, total = pl.pallas_call(
        place_kernel,
        out_shape=(
            jax.ShapeDtypeStruct((rows, G), f32),
            jax.ShapeDtypeStruct((2 * nblk, LANES), f32),
            jax.ShapeDtypeStruct((1,), i32),
        ),
        in_specs=[spec(VMEM)] * 3,
        out_specs=(spec(pl.ANY), spec(pl.ANY), spec(SMEM)),
        scratch_shapes=[VMEM((rows, G), f32), SMEM((SUB, LANES), i32), dma, dma((chunks,)), dma],
        compiler_params=pltpu.CompilerParams(vmem_limit_bytes=limit),
        name="place",
    )(where, peak, buf)
    peak = jnp.swapaxes(peak.reshape(nblk, 2, LANES), 0, 1).reshape(2, G)
    return peak, clones, total.reshape(())


def solution(mesh):
    return jax.shard_map(
        functools.partial(body, mesh.shape["view"], mesh.shape["gauss"]),
        mesh=mesh,
        in_specs=(
            P(None, "gauss"),
            P(None, "gauss"),
            P(None, "gauss"),
            P(None, "gauss"),
            P("view", None, "gauss"),
            P("view", "gauss"),
            P("gauss"),
            P("view", None, None),
            P("view", None),
            P("view"),
        ),
        out_specs=(P(None, "gauss"), P(None, "gauss"), P()),
        check_vma=False,
    )
```

```python
import functools

import jax
import jax.numpy as jnp
from jax import lax
from jax.experimental import pallas as pl
from jax.experimental.pallas import tpu as pltpu
from jax.sharding import PartitionSpec as P

LANES = 128
SUB = 8
TILES = 8
VMEM = pltpu.VMEM
SMEM = pltpu.SMEM
HBM = pltpu.HBM
MESH = pl.DeviceIdType.MESH


def spec(space):
    return pl.BlockSpec(memory_space=space)


def peer(view, gauss):
    return {"view": view, "gauss": gauss}


def quat_factor(scales, quats):
    w, x, y, z = quats
    inv = lax.rsqrt(w * w + x * x + y * y + z * z + 0.25)
    w, x, y, z = (w * inv, x * inv, y * inv, z * inv)
    rq = [
        [1 - 2 * (y * y + z * z), 2 * (x * y - w * z), 2 * (x * z + w * y)],
        [2 * (x * y + w * z), 1 - 2 * (x * x + z * z), 2 * (y * z - w * x)],
        [2 * (x * z - w * y), 2 * (y * z + w * x), 1 - 2 * (x * x + y * y)],
    ]
    return [[rq[i][j] * scales[j] for j in range(3)] for i in range(3)]


def view_lam(means, factor, rot, trans, focal_v):
    point = [
        rot[i][0] * means[0] + rot[i][1] * means[1] + rot[i][2] * means[2] + trans[i]
        for i in range(3)
    ]
    inv = 1.0 / jnp.maximum(point[2], 1.0)
    j00 = focal_v * inv
    j02 = -(j00 * point[0]) * inv
    j12 = -(j00 * point[1]) * inv
    first = [j00 * rot[0][j] + j02 * rot[2][j] for j in range(3)]
    second = [j00 * rot[1][j] + j12 * rot[2][j] for j in range(3)]
    prow = [sum((first[j] * factor[j][k] for j in range(3))) for k in range(3)]
    qrow = [sum((second[j] * factor[j][k] for j in range(3))) for k in range(3)]
    a_val = prow[0] * prow[0] + prow[1] * prow[1] + prow[2] * prow[2] + 0.3
    c_val = qrow[0] * qrow[0] + qrow[1] * qrow[1] + qrow[2] * qrow[2] + 0.3
    b_val = prow[0] * qrow[0] + prow[1] * qrow[1] + prow[2] * qrow[2]
    half = 0.5 * (a_val - c_val)
    disc = half * half + b_val * b_val + 0.01
    return 0.5 * (a_val + c_val) + disc * lax.rsqrt(disc)


YO = (0, 1, 3, 2)
ZO = (0, 1, 7, 2, 6, 3, 5, 4)
GROUPS = (2, 2, 4, 8, 8, 8)


def pick(table, index):
    out = jnp.full(index.shape, table[0], jnp.int32)
    for i in range(1, len(table)):
        out = jnp.where(index == i, table[i], out)
    return out


def main_kernel(
    V, S, views, rots_h, trns_h, foc_h, mask_h, means_h, scales_h, quats_h, attrs_h, grad_h, vis_h,
    buf, peak, where_out,
    rots, trns, foc, mask, means, scales, quats, grad, vis, fac, x, enc, g, split, packed, send, cnt, counts,
    local, halves, merged, whole, lsem, csend, crecv, psend, precv,
    fsend, frecv, xsend, xrecv, hsend, hrecv, msend, mrecv,
):
    v, s = lax.axis_index("view"), lax.axis_index("gauss")
    nblk = mask.shape[0]
    per = nblk // S
    Z = len(ZO)
    Y = len(YO)
    X = V // 2
    core = lax.rem(v, 2)
    chip = lax.div(v, 2)
    mate = v + 1 - 2 * core
    nxt = 2 * lax.rem(chip + 1, X) + core
    prv = 2 * lax.rem(chip + X - 1, X) + core
    opp = 2 * lax.rem(chip + 2, X) + core
    y, z = lax.div(s, Z), lax.rem(s, Z)
    i32, f32, bf16 = jnp.int32, jnp.float32, jnp.bfloat16

    def dest(p):
        return lax.rem(y + YO[p // Z], Y) * Z + lax.rem(z + ZO[p % Z], Z)

    bar = pltpu.get_barrier_semaphore()
    for p in range(1, S):
        pl.semaphore_signal(bar, inc=1, device_id=peer(v, dest(p)), device_id_type=MESH)
    for to in (mate, nxt, prv, opp):
        pl.semaphore_signal(bar, inc=1, device_id=peer(to, s), device_id_type=MESH)

    loads = [
        pltpu.make_async_copy(a, b, lsem.at[i])
        for i, (a, b) in enumerate((
            (mask_h, mask), (means_h, means), (scales_h, scales), (quats_h, quats),
            (grad_h, grad), (vis_h, vis), (rots_h, rots), (trns_h, trns), (foc_h, foc),
        ))
    ]
    for c in loads:
        c.start()

    def tiles(act):
        for t in range(1, TILES):
            @pl.when(v == t)
            def _():
                n = 6 if t < TILES - 1 else 1
                act(pltpu.make_async_copy(
                    attrs_h.at[pl.ds((t - 1) * SUB, n), :], x.at[pl.ds(0, n), :], lsem.at[9]
                ))
                if t > 1:
                    act(pltpu.make_async_copy(
                        attrs_h.at[pl.ds((t - 2) * SUB + 6, 2), :], x.at[pl.ds(6, 2), :], lsem.at[10]
                    ))

    loads[0].wait()
    m = mask[...]
    cnt[...] = jnp.full((1, LANES), jnp.sum(m), i32)
    step = 2 * SUB

    def lines(ref, i, count, c):
        return ref[pl.ds(i * step * count + c, step, stride=count), :]

    for i in (1, 2, 3):
        loads[i].wait()

    def shape(i, carry):
        rows = pl.ds(pl.multiple_of(i * step, step), step)
        factor = quat_factor(
            [scales[rows, c, :] for c in range(3)], [lines(quats, i, 4, c) for c in range(4)]
        )
        for c in range(3):
            fac[9 + c, rows, :] = means[rows, c, :]
            for e in range(3):
                fac[3 * c + e, rows, :] = factor[c][e]
        return carry

    lax.fori_loop(0, nblk // step, shape, 0)
    for i in range(4, 9):
        loads[i].wait()
    tiles(lambda c: c.start())
    for u in range(views):
        rot = [[rots[a, u, b] for b in range(3)] for a in range(3)]
        trans = [trns[u, a] for a in range(3)]
        fl = foc[u]

        def look(i, carry):
            rows = pl.ds(pl.multiple_of(i * step, step), step)
            factor = [[fac[3 * a + b, rows, :] for b in range(3)] for a in range(3)]
            lam = view_lam([fac[9 + c, rows, :] for c in range(3)], factor, rot, trans, fl)
            seen = lines(vis, i, views, u) != 0
            g0, g1 = (grad[u, pl.ds(i * step * 2 + c, step, stride=2), :] for c in range(2))
            for c, value in enumerate((g0 * g0 + g1 * g1, lam)):
                at = pl.ds(i * step * 2 + c, step, stride=2)
                value = jnp.where(seen, value, 0.0)
                local[at, :] = value if u == 0 else jnp.maximum(local[at, :], value)
            return carry

        lax.fori_loop(0, nblk // step, look, 0)

    started = []

    def remote(a, b, ss, rs, to):
        return pltpu.make_async_remote_copy(
            src_ref=a, dst_ref=b, send_sem=ss, recv_sem=rs, device_id=to, device_id_type=MESH
        )

    def go(copy):
        copy.start()
        started.append(copy)
        return copy

    pl.semaphore_wait(bar, S + 3)
    tally = [
        go(remote(cnt, counts.at[pl.ds(p, 1), :], csend.at[p], crecv.at[p], peer(v, dest(p))))
        for p in range(1, S)
    ]
    mine = pl.ds(pl.multiple_of(core * nblk, nblk), nblk)
    other = pl.ds(pl.multiple_of((1 - core) * nblk, nblk), nblk)
    pair = go(remote(local.at[other, :], halves, psend.at[0], precv.at[0], peer(mate, s)))
    counts[0:1, :] = cnt[...]

    lane = lax.broadcasted_iota(i32, (nblk, LANES), 1)
    row = lax.broadcasted_iota(i32, (nblk, LANES), 0)
    mb = m.astype(bf16)
    before = (row < lane).astype(bf16)
    above = (row > lane).astype(bf16)
    dot = functools.partial(jnp.dot, preferred_element_type=f32)
    ones = jnp.ones((LANES, LANES), bf16)
    rank = dot(mb, before).astype(i32)
    size = dot(mb, ones).astype(i32)
    base = dot(dot(above, mb).astype(bf16), ones).astype(i32)
    flat = lax.dot_general(
        jnp.ones((SUB, LANES), bf16), mb, (((1,), (1,)), ((), ())), preferred_element_type=f32
    )
    starts = dot(flat.astype(bf16), before).astype(i32)
    code = jnp.where(m == 1, 65536 + (lane - rank) * 256 + lane, 0)
    bit = 1
    while bit < LANES:
        moved = pltpu.roll(code, LANES - bit, 1)
        goes = (moved & (bit * 256)) != 0
        stays = (code & (bit * 256)) == 0
        code = jnp.where(goes, moved, jnp.where(stays, code, 0))
        bit *= 2
    turn = (lane - base) & (LANES - 1)
    src = jnp.take_along_axis(code & (LANES - 1), turn, axis=1)
    valid = turn < size
    idx = jnp.where(valid, src, 0)
    enc[...] = jnp.where(valid, src, -1)
    head = lane >= (base & (LANES - 1))
    low, high = valid & head, valid & jnp.logical_not(head)


    pair.wait_recv()
    merged[...] = jnp.maximum(local[mine, :], halves[...])
    spread = [
        go(remote(merged, whole.at[k], psend.at[1 + k], precv.at[1 + k], peer(to, s)))
        for k, to in enumerate((nxt, prv, opp))
    ]

    tiles(lambda c: c.wait())

    @pl.when(v > 0)
    def _():
        def gather(b, carry):
            e = jnp.broadcast_to(enc[pl.ds(b, 1), :], (SUB, LANES))
            cols = pl.ds(pl.multiple_of(b * LANES, LANES), LANES)
            got = jnp.take_along_axis(x[:, cols], jnp.maximum(e, 0), axis=1)
            g[b] = got
            return carry

        lax.fori_loop(0, nblk, gather, 0, unroll=8)

    def put(final, value):
        g[:, (final + 6) % SUB, :] = jnp.take_along_axis(value, idx, axis=1)

    @pl.when(v == 0)
    def _():
        for c in range(3):
            put(c, means[:, c, :])
            put(3 + c, scales[:, c, :])
        for c in range(2):
            put(6 + c, quats[pl.ds(c, nblk, stride=4), :])

    @pl.when(v == 1)
    def _():
        for c in range(2):
            put(c, quats[pl.ds(2 + c, nblk, stride=4), :])

    def cut(c):
        value = g[:, (c + 6) % SUB, :]
        for part, keep in enumerate((low, high)):
            rest = jnp.where(keep, value, 0.0)
            for i in range(3):
                top = rest.astype(bf16)
                split[(2 * i + part) * nblk:(2 * i + part + 1) * nblk, c * LANES:(c + 1) * LANES] = top
                rest = rest - top.astype(f32)

    at = starts[0:1, :] >> 7
    hot = jnp.concatenate([(row == at).astype(bf16), (row == at + 1).astype(bf16)] * 3, axis=1)

    def pack(*finals):
        for c in finals:
            cut(c)
        lo, hi = finals[0], finals[-1] + 1
        moved = dot(hot, split[:, lo * LANES:hi * LANES])
        for c in finals:
            packed[:, c, :] = moved[:, (c - lo) * LANES:(c - lo + 1) * LANES]

    full = remote(peak.at[mine, :], peak.at[mine, :], psend.at[4], precv.at[4], peer(mate, s))

    def finish():
        for c in spread:
            c.wait_recv()
        best = merged[...]
        for k in range(3):
            best = jnp.maximum(best, whole[k])
        odd = (lax.broadcasted_iota(i32, best.shape, 0) & 1) == 1
        peak[mine, :] = jnp.sqrt(best) * jnp.where(odd, 3.0, 1.0)
        full.start()
        full.wait_recv()

    pack(0, 1, 2)

    @pl.when(v < TILES - 1)
    def _():
        pack(3, 4, 5, 6, 7)

    @pl.when(v == TILES - 1)
    def _():
        packed[:, 5:, :] = jnp.zeros((nblk, 3, LANES), f32)
        finish()
        for c in range(2):
            put(3 + c, peak[pl.ds(c, nblk, stride=2), :])
        pack(3, 4)

    def source(p):
        return ((y - pick(YO, p >> 3)) & (Y - 1)) * Z + ((z - pick(ZO, p & 7)) & (Z - 1))

    p32 = lax.broadcasted_iota(i32, (S, LANES), 0)
    lower = source(p32) < s
    for c in tally:
        c.wait_recv()
    tot = counts[...]
    blocks = (tot + (LANES - 1)) >> 7
    offset = jnp.sum(jnp.where(lower, blocks, 0), axis=0)[0]
    for p in range(S):
        first = (dest(p) - offset) & (S - 1)
        for w in range(per):
            send[p * per + w] = packed[first + S * w]

    fars = [None]
    for p in range(1, S):
        fars.append(go(remote(
            send.at[pl.ds(p * per, per)], buf.at[v, pl.ds(p * per, per)],
            fsend.at[p], frecv.at[p], peer(v, dest(p)),
        )))
    own = pltpu.make_async_copy(send.at[pl.ds(0, per)], buf.at[v, pl.ds(0, per)], fsend.at[0])
    own.start()

    @pl.when(v < TILES - 1)
    def _():
        finish()

    started.append(full)
    pr = lax.broadcasted_iota(i32, (S, S), 0)
    pc = lax.broadcasted_iota(i32, (S, S), 1)
    less = (source(pc) < source(pr)).astype(bf16)
    offs = dot(less, blocks.astype(bf16)).astype(i32)
    k = lax.broadcasted_iota(i32, (S, LANES), 1) * S + s
    here = (k >= offs) & (k < offs + blocks)
    spot = jnp.where(here, p32 * per + ((k - offs) >> 5) + 1, 0)
    found = jnp.sum(spot, axis=0, keepdims=True) - 1
    total = jnp.sum(tot, axis=0, keepdims=True)
    sub = lax.broadcasted_iota(i32, (SUB, LANES), 0)
    where_out[...] = jnp.where(sub == 0, found, total)

    edges = [0]
    for n in GROUPS:
        edges.append(edges[-1] + n)
    N = len(GROUPS)

    def group(owner, i, half=None):
        first, size = edges[i] * per, GROUPS[i] * per
        if half is not None:
            size //= 2
            first += half * size
        return buf.at[owner, pl.ds(first, size)]

    def ring(i, way):
        return remote(group(v, i), group(v, i), xsend.at[way, i], xrecv.at[way, i], peer((nxt, prv)[way], s))

    def relay(i, way):
        ref = group((prv, nxt)[way], i, way)
        return remote(ref, ref, hsend.at[way, i], hrecv.at[way, i], peer((nxt, prv)[way], s))

    def beside(i, q):
        ref = group((v, prv, nxt, opp)[q], i)
        return remote(ref, ref, msend.at[q, i], mrecv.at[q, i], peer(mate, s))

    rings, relays, besides = {}, {}, {}
    for i in range(N + 2):
        if i < N:
            for p in range(edges[i], edges[i + 1]):
                if p:
                    fars[p].wait_recv()
                else:
                    own.wait()
            for way in range(2):
                rings[i, way] = go(ring(i, way))
            besides[i, 0] = go(beside(i, 0))
        if 1 <= i <= N:
            for way in range(2):
                rings[i - 1, way].wait_recv()
                relays[i - 1, way] = go(relay(i - 1, way))
                besides[i - 1, 1 + way] = go(beside(i - 1, 1 + way))
        if i >= 2:
            for way in range(2):
                relays[i - 2, way].wait_recv()
            besides[i - 2, 3] = go(beside(i - 2, 3))
    for c in besides.values():
        c.wait_recv()
    for c in started:
        c.wait_send()


def place_kernel(idx_v, peak_in, buf, clones, peak, total, out, idx, isem, osem, psem):
    rows = clones.shape[0]
    slots = out.shape[1] // LANES
    chunks = osem.shape[0]
    fetch = pltpu.make_async_copy(idx_v, idx, isem)
    fetch.start()
    top = pltpu.make_async_copy(peak_in, peak, psem)
    top.start()
    fetch.wait()
    total[0] = idx[1, 0]
    each = slots // chunks
    outs = []
    for c in range(chunks):
        def one(q, carry):
            r = idx[0, q]
            on = r >= 0
            r = jnp.maximum(r, 0)
            cols = pl.ds(pl.multiple_of(q * LANES, LANES), LANES)
            for i in range(TILES):
                n = min(rows - i * SUB, SUB)
                out[i * SUB:i * SUB + n, cols] = jnp.where(on, buf[i, r], 0.0)[:n]
            return carry

        lax.fori_loop(c * each, (c + 1) * each, one, 0, unroll=4)
        cols = pl.ds(c * each * LANES, each * LANES)
        cp = pltpu.make_async_copy(out.at[:, cols], clones.at[:, cols], osem.at[c])
        cp.start()
        outs.append(cp)
    for cp in outs:
        cp.wait()
    top.wait()


def body(V, S, means, scales, quats, attrs, grad_screen, visible, clone_mask, rotation, shift, focal):
    G = clone_mask.shape[0]
    nblk = G // LANES
    views = grad_screen.shape[0]
    rows = means.shape[0] + scales.shape[0] + quats.shape[0] + attrs.shape[0] + 2
    f32, i32 = jnp.float32, jnp.int32

    def lines(a):
        a = a.reshape(a.shape[:-1] + (nblk, LANES))
        return jnp.swapaxes(a, -3, -2)

    dma = pltpu.SemaphoreType.DMA
    N = len(GROUPS)
    limit = 32 * 1024 * 1024
    buf, peak, where = pl.pallas_call(
        functools.partial(main_kernel, V, S, views),
        out_shape=(
            VMEM((V, nblk, SUB, LANES), f32), VMEM((2 * nblk, LANES), f32), VMEM((SUB, LANES), i32),
        ),
        in_specs=[spec(HBM)] * 10,
        out_specs=(spec(VMEM),) * 3,
        scratch_shapes=[
            SMEM((3, views, 3), f32),
            SMEM((views, 3), f32),
            SMEM((views,), f32),
            VMEM((nblk, LANES), i32),
            VMEM((nblk, 3, LANES), f32),
            VMEM((nblk, 3, LANES), f32),
            VMEM((4 * nblk, LANES), f32),
            VMEM((views, 2 * nblk, LANES), f32),
            VMEM((views * nblk, LANES), i32),
            VMEM((12, nblk, LANES), f32),
            VMEM((SUB, G), f32),
            VMEM((nblk, LANES), i32),
            VMEM((nblk, SUB, LANES), f32),
            VMEM((6 * nblk, SUB * LANES), jnp.bfloat16),
            VMEM((nblk, SUB, LANES), f32),
            VMEM((nblk, SUB, LANES), f32),
            VMEM((1, LANES), i32),
            VMEM((S, LANES), i32),
            VMEM((2 * nblk, LANES), f32),
            VMEM((nblk, LANES), f32),
            VMEM((nblk, LANES), f32),
            VMEM((3, nblk, LANES), f32),
            dma((11,)), dma((S,)), dma((S,)), dma((5,)), dma((5,)),
            dma((S,)), dma((S,)), dma((2, N)), dma((2, N)), dma((2, N)), dma((2, N)),
            dma((4, N)), dma((4, N)),
        ],
        compiler_params=pltpu.CompilerParams(
            collective_id=0, has_side_effects=True, vmem_limit_bytes=limit
        ),
        name="main",
    )(*(
        pltpu.with_memory_space_constraint(a, HBM)
        for a in (
            jnp.transpose(rotation, (1, 0, 2)), shift, focal, clone_mask.reshape(nblk, LANES),
            lines(means), lines(scales), lines(quats).reshape(-1, LANES), attrs,
            lines(grad_screen).reshape(views, -1, LANES), lines(visible).reshape(-1, LANES),
        )
    ))
    chunks = 8
    clones, peak, total = pl.pallas_call(
        place_kernel,
        out_shape=(
            jax.ShapeDtypeStruct((rows, G), f32),
            jax.ShapeDtypeStruct((2 * nblk, LANES), f32),
            jax.ShapeDtypeStruct((1,), i32),
        ),
        in_specs=[spec(VMEM)] * 3,
        out_specs=(spec(pl.ANY), spec(pl.ANY), spec(SMEM)),
        scratch_shapes=[VMEM((rows, G), f32), SMEM((SUB, LANES), i32), dma, dma((chunks,)), dma],
        compiler_params=pltpu.CompilerParams(vmem_limit_bytes=limit),
        name="place",
    )(where, peak, buf)
    peak = jnp.swapaxes(peak.reshape(nblk, 2, LANES), 0, 1).reshape(2, G)
    return peak, clones, total.reshape(())


def solution(mesh):
    return jax.shard_map(
        functools.partial(body, mesh.shape["view"], mesh.shape["gauss"]),
        mesh=mesh,
        in_specs=(
            P(None, "gauss"),
            P(None, "gauss"),
            P(None, "gauss"),
            P(None, "gauss"),
            P("view", None, "gauss"),
            P("view", "gauss"),
            P("gauss"),
            P("view", None, None),
            P("view", None),
            P("view"),
        ),
        out_specs=(P(None, "gauss"), P(None, "gauss"), P()),
        check_vma=False,
    )
```

```python
import functools

import jax
import jax.numpy as jnp
from jax import lax
from jax.experimental import pallas as pl
from jax.experimental.pallas import tpu as pltpu
from jax.sharding import PartitionSpec as P

LANES = 128
SUB = 8
TILES = 8
VMEM = pltpu.VMEM
SMEM = pltpu.SMEM
HBM = pltpu.HBM
MESH = pl.DeviceIdType.MESH


def spec(space):
    return pl.BlockSpec(memory_space=space)


def peer(view, gauss):
    return {"view": view, "gauss": gauss}


def quat_factor(scales, quats):
    w, x, y, z = quats
    inv = lax.rsqrt(w * w + x * x + y * y + z * z + 0.25)
    w, x, y, z = (w * inv, x * inv, y * inv, z * inv)
    rq = [
        [1 - 2 * (y * y + z * z), 2 * (x * y - w * z), 2 * (x * z + w * y)],
        [2 * (x * y + w * z), 1 - 2 * (x * x + z * z), 2 * (y * z - w * x)],
        [2 * (x * z - w * y), 2 * (y * z + w * x), 1 - 2 * (x * x + y * y)],
    ]
    return [[rq[i][j] * scales[j] for j in range(3)] for i in range(3)]


def view_lam(means, factor, rot, trans, focal_v):
    point = [
        rot[i][0] * means[0] + rot[i][1] * means[1] + rot[i][2] * means[2] + trans[i]
        for i in range(3)
    ]
    inv = 1.0 / jnp.maximum(point[2], 1.0)
    j00 = focal_v * inv
    j02 = -(j00 * point[0]) * inv
    j12 = -(j00 * point[1]) * inv
    first = [j00 * rot[0][j] + j02 * rot[2][j] for j in range(3)]
    second = [j00 * rot[1][j] + j12 * rot[2][j] for j in range(3)]
    prow = [sum((first[j] * factor[j][k] for j in range(3))) for k in range(3)]
    qrow = [sum((second[j] * factor[j][k] for j in range(3))) for k in range(3)]
    a_val = prow[0] * prow[0] + prow[1] * prow[1] + prow[2] * prow[2] + 0.3
    c_val = qrow[0] * qrow[0] + qrow[1] * qrow[1] + qrow[2] * qrow[2] + 0.3
    b_val = prow[0] * qrow[0] + prow[1] * qrow[1] + prow[2] * qrow[2]
    half = 0.5 * (a_val - c_val)
    disc = half * half + b_val * b_val + 0.01
    return 0.5 * (a_val + c_val) + disc * lax.rsqrt(disc)


Y, Z = 4, 8


def near(step):
    y, z = (min(a, n - a) for a, n in zip(step, (Y, Z)))
    return y + z, z


STEPS = sorted(((a, b) for a in range(Y) for b in range(Z)), key=near)
YO, ZO = zip(*STEPS)
GROUPS = (5, 7, 8, 7, 5)
LAG = (2, 4)


def pick(table, index):
    out = jnp.full(index.shape, table[0], jnp.int32)
    for i in range(1, len(table)):
        out = jnp.where(index == i, table[i], out)
    return out


def main_kernel(
    V, S, views, rots_h, trns_h, foc_h, mask_h, means_h, scales_h, quats_h, attrs_h, grad_h, vis_h,
    buf, peak, where_out,
    rots, trns, foc, mask, means, scales, quats, grad, vis, fac, x, enc, g, split, packed, send, cnt, counts,
    local, halves, merged, whole, lsem, csend, crecv, psend, precv,
    fsend, frecv, xsend, xrecv, hsend, hrecv, msend, mrecv,
):
    v, s = lax.axis_index("view"), lax.axis_index("gauss")
    nblk = mask.shape[0]
    per = nblk // S
    X = V // 2
    core = lax.rem(v, 2)
    chip = lax.div(v, 2)
    mate = v + 1 - 2 * core
    nxt = 2 * lax.rem(chip + 1, X) + core
    prv = 2 * lax.rem(chip + X - 1, X) + core
    opp = 2 * lax.rem(chip + 2, X) + core
    y, z = lax.div(s, Z), lax.rem(s, Z)
    i32, f32, bf16 = jnp.int32, jnp.float32, jnp.bfloat16

    def dest(p):
        return lax.rem(y + YO[p], Y) * Z + lax.rem(z + ZO[p], Z)

    bar = pltpu.get_barrier_semaphore()
    for p in range(1, S):
        pl.semaphore_signal(bar, inc=1, device_id=peer(v, dest(p)), device_id_type=MESH)
    for to in (mate, nxt, prv, opp):
        pl.semaphore_signal(bar, inc=1, device_id=peer(to, s), device_id_type=MESH)

    @pl.when(v == V - 1)
    def _():
        for k in range(X - 1):
            pl.semaphore_signal(bar, inc=1, device_id=peer(2 * k, s), device_id_type=MESH)

    loads = [
        pltpu.make_async_copy(a, b, lsem.at[i])
        for i, (a, b) in enumerate((
            (mask_h, mask), (means_h, means), (scales_h, scales), (quats_h, quats),
            (grad_h, grad), (vis_h, vis), (rots_h, rots), (trns_h, trns), (foc_h, foc),
        ))
    ]
    for c in loads:
        c.start()

    def tiles(act):
        for t in range(1, TILES):
            @pl.when(v == t)
            def _():
                n = 6 if t < TILES - 1 else 1
                act(pltpu.make_async_copy(
                    attrs_h.at[pl.ds((t - 1) * SUB, n), :], x.at[pl.ds(0, n), :], lsem.at[9]
                ))
                if t > 1:
                    act(pltpu.make_async_copy(
                        attrs_h.at[pl.ds((t - 2) * SUB + 6, 2), :], x.at[pl.ds(6, 2), :], lsem.at[10]
                    ))

    loads[0].wait()
    m = mask[...]
    cnt[...] = jnp.full((1, LANES), jnp.sum(m), i32)
    step = 2 * SUB

    def lines(ref, i, count, c):
        return ref[pl.ds(i * step * count + c, step, stride=count), :]

    for i in (1, 2, 3):
        loads[i].wait()

    def shape(i, carry):
        rows = pl.ds(pl.multiple_of(i * step, step), step)
        factor = quat_factor(
            [scales[rows, c, :] for c in range(3)], [lines(quats, i, 4, c) for c in range(4)]
        )
        for c in range(3):
            fac[9 + c, rows, :] = means[rows, c, :]
            for e in range(3):
                fac[3 * c + e, rows, :] = factor[c][e]
        return carry

    lax.fori_loop(0, nblk // step, shape, 0)
    for i in range(4, 9):
        loads[i].wait()
    tiles(lambda c: c.start())
    for u in range(views):
        rot = [[rots[a, u, b] for b in range(3)] for a in range(3)]
        trans = [trns[u, a] for a in range(3)]
        fl = foc[u]

        def look(i, carry):
            rows = pl.ds(pl.multiple_of(i * step, step), step)
            factor = [[fac[3 * a + b, rows, :] for b in range(3)] for a in range(3)]
            lam = view_lam([fac[9 + c, rows, :] for c in range(3)], factor, rot, trans, fl)
            seen = lines(vis, i, views, u) != 0
            g0, g1 = (grad[u, pl.ds(i * step * 2 + c, step, stride=2), :] for c in range(2))
            for c, value in enumerate((g0 * g0 + g1 * g1, lam)):
                at = pl.ds(i * step * 2 + c, step, stride=2)
                value = jnp.where(seen, value, 0.0)
                local[at, :] = value if u == 0 else jnp.maximum(local[at, :], value)
            return carry

        lax.fori_loop(0, nblk // step, look, 0)

    started = []

    def remote(a, b, ss, rs, to):
        return pltpu.make_async_remote_copy(
            src_ref=a, dst_ref=b, send_sem=ss, recv_sem=rs, device_id=to, device_id_type=MESH
        )

    def go(copy):
        copy.start()
        started.append(copy)
        return copy

    pl.semaphore_wait(bar, S + 3 + jnp.where((core == 0) & (chip < X - 1), 1, 0))
    tally = [
        go(remote(cnt, counts.at[pl.ds(p, 1), :], csend.at[p], crecv.at[p], peer(v, dest(p))))
        for p in reversed(range(1, S))
    ]
    mine = pl.ds(pl.multiple_of(core * nblk, nblk), nblk)
    last = V - 1
    pair = go(remote(local, halves, psend.at[0], precv.at[0], peer(mate, s)))
    counts[0:1, :] = cnt[...]

    lane = lax.broadcasted_iota(i32, (nblk, LANES), 1)
    row = lax.broadcasted_iota(i32, (nblk, LANES), 0)
    mb = m.astype(bf16)
    before = (row < lane).astype(bf16)
    above = (row > lane).astype(bf16)
    dot = functools.partial(jnp.dot, preferred_element_type=f32)
    ones = jnp.ones((LANES, LANES), bf16)
    rank = dot(mb, before).astype(i32)
    size = dot(mb, ones).astype(i32)
    base = dot(dot(above, mb).astype(bf16), ones).astype(i32)
    flat = lax.dot_general(
        jnp.ones((SUB, LANES), bf16), mb, (((1,), (1,)), ((), ())), preferred_element_type=f32
    )
    starts = dot(flat.astype(bf16), before).astype(i32)
    code = jnp.where(m == 1, 65536 + (lane - rank) * 256 + lane, 0)
    bit = 1
    while bit < LANES:
        moved = pltpu.roll(code, LANES - bit, 1)
        goes = (moved & (bit * 256)) != 0
        stays = (code & (bit * 256)) == 0
        code = jnp.where(goes, moved, jnp.where(stays, code, 0))
        bit *= 2
    turn = (lane - base) & (LANES - 1)
    src = jnp.take_along_axis(code & (LANES - 1), turn, axis=1)
    valid = turn < size
    idx = jnp.where(valid, src, 0)
    enc[...] = jnp.where(valid, src, -1)
    head = lane >= (base & (LANES - 1))
    low, high = valid & head, valid & jnp.logical_not(head)


    pair.wait_recv()
    merged[...] = jnp.maximum(local[...], halves[...])
    spread = []
    for k in range(1, X):
        to = lax.rem(chip + k, X)
        spread.append(go(remote(
            merged.at[mine, :], whole.at[k - 1, mine, :], psend.at[k], precv.at[k + X * core],
            peer(2 * to + jnp.where(to == X - 1, 1, core), s),
        )))

    tiles(lambda c: c.wait())

    @pl.when(v > 0)
    def _():
        def gather(b, carry):
            e = jnp.broadcast_to(enc[pl.ds(b, 1), :], (SUB, LANES))
            cols = pl.ds(pl.multiple_of(b * LANES, LANES), LANES)
            got = jnp.take_along_axis(x[:, cols], jnp.maximum(e, 0), axis=1)
            g[b] = got
            return carry

        lax.fori_loop(0, nblk, gather, 0, unroll=8)

    def put(final, value):
        g[:, (final + 6) % SUB, :] = jnp.take_along_axis(value, idx, axis=1)

    @pl.when(v == 0)
    def _():
        for c in range(3):
            put(c, means[:, c, :])
            put(3 + c, scales[:, c, :])
        for c in range(2):
            put(6 + c, quats[pl.ds(c, nblk, stride=4), :])

    @pl.when(v == 1)
    def _():
        for c in range(2):
            put(c, quats[pl.ds(2 + c, nblk, stride=4), :])

    def cut(c):
        value = g[:, (c + 6) % SUB, :]
        for part, keep in enumerate((low, high)):
            rest = jnp.where(keep, value, 0.0)
            for i in range(3):
                top = rest.astype(bf16)
                split[(2 * i + part) * nblk:(2 * i + part + 1) * nblk, c * LANES:(c + 1) * LANES] = top
                rest = rest - top.astype(f32)

    at = starts[0:1, :] >> 7
    hot = jnp.concatenate([(row == at).astype(bf16), (row == at + 1).astype(bf16)] * 3, axis=1)

    def pack(*finals):
        for c in finals:
            cut(c)
        lo, hi = finals[0], finals[-1] + 1
        moved = dot(hot, split[:, lo * LANES:hi * LANES])
        for c in finals:
            packed[:, c, :] = moved[:, (c - lo) * LANES:(c - lo + 1) * LANES]

    full = remote(peak.at[mine, :], peak.at[mine, :], psend.at[X + 1], precv.at[X], peer(mate, s))
    extra = remote(peak, peak, psend.at[X], precv.at[X], peer(mate, s))

    def arrive(half):
        for k in range(1, X):
            ref = whole.at[k - 1, pl.ds(half * nblk, nblk), :]
            remote(ref, ref, psend.at[k], precv.at[k + X * half], peer(mate, s)).wait_recv()

    def finish(rows):
        best = merged[rows, :]
        for k in range(X - 1):
            best = jnp.maximum(best, whole[k, rows, :])
        odd = (lax.broadcasted_iota(i32, best.shape, 0) & 1) == 1
        peak[rows, :] = jnp.sqrt(best) * jnp.where(odd, 3.0, 1.0)

    pack(0, 1, 2)

    @pl.when(v < TILES - 1)
    def _():
        pack(3, 4, 5, 6, 7)

    @pl.when(v == TILES - 1)
    def _():
        packed[:, 5:, :] = jnp.zeros((nblk, 3, LANES), f32)
        arrive(0)
        arrive(1)
        finish(pl.ds(0, 2 * nblk))
        extra.start()
        for c in range(2):
            put(3 + c, peak[pl.ds(c, nblk, stride=2), :])
        pack(3, 4)

    def source(p):
        return ((y - pick(YO, p)) & (Y - 1)) * Z + ((z - pick(ZO, p)) & (Z - 1))

    p32 = lax.broadcasted_iota(i32, (S, LANES), 0)
    lower = source(p32) < s
    for c in tally:
        c.wait_recv()
    tot = counts[...]
    blocks = (tot + (LANES - 1)) >> 7
    offset = jnp.sum(jnp.where(lower, blocks, 0), axis=0)[0]
    for p in range(S):
        first = (dest(p) - offset) & (S - 1)
        for w in range(per):
            send[p * per + w] = packed[first + S * w]

    fars = [None]
    for p in range(1, S):
        fars.append(go(remote(
            send.at[pl.ds(p * per, per)], buf.at[v, pl.ds(p * per, per)],
            fsend.at[p], frecv.at[p], peer(v, dest(p)),
        )))
    own = pltpu.make_async_copy(send.at[pl.ds(0, per)], buf.at[v, pl.ds(0, per)], fsend.at[0])
    own.start()

    for half in range(2):
        @pl.when((chip < X - 1) & (core == half))
        def _():
            arrive(half)
            finish(mine)
            full.start()
            full.wait()

    @pl.when(v == last - 1)
    def _():
        extra.wait_recv()

    @pl.when(v == last)
    def _():
        extra.wait_send()

    pr = lax.broadcasted_iota(i32, (S, S), 0)
    pc = lax.broadcasted_iota(i32, (S, S), 1)
    less = (source(pc) < source(pr)).astype(bf16)
    offs = dot(less, blocks.astype(bf16)).astype(i32)
    k = lax.broadcasted_iota(i32, (S, LANES), 1) * S + s
    here = (k >= offs) & (k < offs + blocks)
    spot = jnp.where(here, p32 * per + ((k - offs) >> 5) + 1, 0)
    found = jnp.sum(spot, axis=0, keepdims=True) - 1
    total = jnp.sum(tot, axis=0, keepdims=True)
    sub = lax.broadcasted_iota(i32, (SUB, LANES), 0)
    where_out[...] = jnp.where(sub == 0, found, total)

    edges = [0]
    for n in GROUPS:
        edges.append(edges[-1] + n)
    N = len(GROUPS)

    def group(owner, i, half=None):
        first, size = edges[i] * per, GROUPS[i] * per
        if half is not None:
            size //= 2
            first += half * size
        return buf.at[owner, pl.ds(first, size)]

    def ring(i, way):
        return remote(group(v, i), group(v, i), xsend.at[way, i], xrecv.at[way, i], peer((nxt, prv)[way], s))

    def relay(i, way):
        ref = group((prv, nxt)[way], i, way)
        return remote(ref, ref, hsend.at[way, i], hrecv.at[way, i], peer((nxt, prv)[way], s))

    def beside(i, q):
        ref = group((v, prv, nxt, opp)[q], i)
        return remote(ref, ref, msend.at[q, i], mrecv.at[q, i], peer(mate, s))

    rings, relays, besides = {}, {}, {}
    for i in range(N + LAG[1]):
        if i < N:
            for p in range(edges[i], edges[i + 1]):
                if p:
                    fars[p].wait_recv()
                else:
                    own.wait()
            for way in range(2):
                rings[i, way] = go(ring(i, way))
            besides[i, 0] = go(beside(i, 0))
        j = i - LAG[0]
        if 0 <= j < N:
            for way in range(2):
                rings[j, way].wait_recv()
                relays[j, way] = go(relay(j, way))
            for way in range(2):
                besides[j, 1 + way] = go(beside(j, 1 + way))
        j = i - LAG[1]
        if 0 <= j < N:
            for way in range(2):
                relays[j, way].wait_recv()
            besides[j, 3] = go(beside(j, 3))
    for c in besides.values():
        c.wait_recv()
    for c in started:
        c.wait_send()


def place_kernel(idx_v, peak_in, buf, clones, peak, total, out, idx, isem, osem, psem):
    rows = clones.shape[0]
    slots = out.shape[1] // LANES
    chunks = osem.shape[0]
    fetch = pltpu.make_async_copy(idx_v, idx, isem)
    fetch.start()
    top = pltpu.make_async_copy(peak_in, peak, psem)
    top.start()
    fetch.wait()
    total[0] = idx[1, 0]
    each = slots // chunks
    outs = []
    for c in range(chunks):
        def one(q, carry):
            r = idx[0, q]
            on = r >= 0
            r = jnp.maximum(r, 0)
            cols = pl.ds(pl.multiple_of(q * LANES, LANES), LANES)
            for i in range(TILES):
                n = min(rows - i * SUB, SUB)
                out[i * SUB:i * SUB + n, cols] = jnp.where(on, buf[i, r], 0.0)[:n]
            return carry

        lax.fori_loop(c * each, (c + 1) * each, one, 0, unroll=4)
        cols = pl.ds(c * each * LANES, each * LANES)
        cp = pltpu.make_async_copy(out.at[:, cols], clones.at[:, cols], osem.at[c])
        cp.start()
        outs.append(cp)
    for cp in outs:
        cp.wait()
    top.wait()


def body(V, S, means, scales, quats, attrs, grad_screen, visible, clone_mask, rotation, shift, focal):
    G = clone_mask.shape[0]
    nblk = G // LANES
    views = grad_screen.shape[0]
    rows = means.shape[0] + scales.shape[0] + quats.shape[0] + attrs.shape[0] + 2
    f32, i32 = jnp.float32, jnp.int32

    def lines(a):
        a = a.reshape(a.shape[:-1] + (nblk, LANES))
        return jnp.swapaxes(a, -3, -2)

    dma = pltpu.SemaphoreType.DMA
    N = len(GROUPS)
    limit = 32 * 1024 * 1024
    buf, peak, where = pl.pallas_call(
        functools.partial(main_kernel, V, S, views),
        out_shape=(
            VMEM((V, nblk, SUB, LANES), f32), VMEM((2 * nblk, LANES), f32), VMEM((SUB, LANES), i32),
        ),
        in_specs=[spec(HBM)] * 10,
        out_specs=(spec(VMEM),) * 3,
        scratch_shapes=[
            SMEM((3, views, 3), f32),
            SMEM((views, 3), f32),
            SMEM((views,), f32),
            VMEM((nblk, LANES), i32),
            VMEM((nblk, 3, LANES), f32),
            VMEM((nblk, 3, LANES), f32),
            VMEM((4 * nblk, LANES), f32),
            VMEM((views, 2 * nblk, LANES), f32),
            VMEM((views * nblk, LANES), i32),
            VMEM((12, nblk, LANES), f32),
            VMEM((SUB, G), f32),
            VMEM((nblk, LANES), i32),
            VMEM((nblk, SUB, LANES), f32),
            VMEM((6 * nblk, SUB * LANES), jnp.bfloat16),
            VMEM((nblk, SUB, LANES), f32),
            VMEM((nblk, SUB, LANES), f32),
            VMEM((1, LANES), i32),
            VMEM((S, LANES), i32),
            VMEM((2 * nblk, LANES), f32),
            VMEM((2 * nblk, LANES), f32),
            VMEM((2 * nblk, LANES), f32),
            VMEM((V // 2 - 1, 2 * nblk, LANES), f32),
            dma((11,)), dma((S,)), dma((S,)), dma((V,)), dma((V,)),
            dma((S,)), dma((S,)), dma((2, N)), dma((2, N)), dma((2, N)), dma((2, N)),
            dma((4, N)), dma((4, N)),
        ],
        compiler_params=pltpu.CompilerParams(
            collective_id=0, has_side_effects=True, vmem_limit_bytes=limit
        ),
        name="main",
    )(*(
        pltpu.with_memory_space_constraint(a, HBM)
        for a in (
            jnp.transpose(rotation, (1, 0, 2)), shift, focal, clone_mask.reshape(nblk, LANES),
            lines(means), lines(scales), lines(quats).reshape(-1, LANES), attrs,
            lines(grad_screen).reshape(views, -1, LANES), lines(visible).reshape(-1, LANES),
        )
    ))
    chunks = 8
    clones, peak, total = pl.pallas_call(
        place_kernel,
        out_shape=(
            jax.ShapeDtypeStruct((rows, G), f32),
            jax.ShapeDtypeStruct((2 * nblk, LANES), f32),
            jax.ShapeDtypeStruct((1,), i32),
        ),
        in_specs=[spec(VMEM)] * 3,
        out_specs=(spec(pl.ANY), spec(pl.ANY), spec(SMEM)),
        scratch_shapes=[VMEM((rows, G), f32), SMEM((SUB, LANES), i32), dma, dma((chunks,)), dma],
        compiler_params=pltpu.CompilerParams(vmem_limit_bytes=limit),
        name="place",
    )(where, peak, buf)
    peak = jnp.swapaxes(peak.reshape(nblk, 2, LANES), 0, 1).reshape(2, G)
    return peak, clones, total.reshape(())


def solution(mesh):
    return jax.shard_map(
        functools.partial(body, mesh.shape["view"], mesh.shape["gauss"]),
        mesh=mesh,
        in_specs=(
            P(None, "gauss"),
            P(None, "gauss"),
            P(None, "gauss"),
            P(None, "gauss"),
            P("view", None, "gauss"),
            P("view", "gauss"),
            P("gauss"),
            P("view", None, None),
            P("view", None),
            P("view"),
        ),
        out_specs=(P(None, "gauss"), P(None, "gauss"), P()),
        check_vma=False,
    )
```

```python
import functools

import jax
import jax.numpy as jnp
from jax import lax
from jax.experimental import pallas as pl
from jax.experimental.pallas import tpu as pltpu
from jax.sharding import PartitionSpec as P

LANES = 128
SUB = 8
TILES = 8
VMEM = pltpu.VMEM
SMEM = pltpu.SMEM
HBM = pltpu.HBM
MESH = pl.DeviceIdType.MESH


def spec(space):
    return pl.BlockSpec(memory_space=space)


def peer(view, gauss):
    return {"view": view, "gauss": gauss}


def quat_factor(scales, quats):
    w, x, y, z = quats
    inv = lax.rsqrt(w * w + x * x + y * y + z * z + 0.25)
    w, x, y, z = (w * inv, x * inv, y * inv, z * inv)
    rq = [
        [1 - 2 * (y * y + z * z), 2 * (x * y - w * z), 2 * (x * z + w * y)],
        [2 * (x * y + w * z), 1 - 2 * (x * x + z * z), 2 * (y * z - w * x)],
        [2 * (x * z - w * y), 2 * (y * z + w * x), 1 - 2 * (x * x + y * y)],
    ]
    return [[rq[i][j] * scales[j] for j in range(3)] for i in range(3)]


def view_lam(means, factor, rot, trans, focal_v):
    point = [
        rot[i][0] * means[0] + rot[i][1] * means[1] + rot[i][2] * means[2] + trans[i]
        for i in range(3)
    ]
    inv = 1.0 / jnp.maximum(point[2], 1.0)
    j00 = focal_v * inv
    j02 = -(j00 * point[0]) * inv
    j12 = -(j00 * point[1]) * inv
    first = [j00 * rot[0][j] + j02 * rot[2][j] for j in range(3)]
    second = [j00 * rot[1][j] + j12 * rot[2][j] for j in range(3)]
    prow = [sum((first[j] * factor[j][k] for j in range(3))) for k in range(3)]
    qrow = [sum((second[j] * factor[j][k] for j in range(3))) for k in range(3)]
    a_val = prow[0] * prow[0] + prow[1] * prow[1] + prow[2] * prow[2] + 0.3
    c_val = qrow[0] * qrow[0] + qrow[1] * qrow[1] + qrow[2] * qrow[2] + 0.3
    b_val = prow[0] * qrow[0] + prow[1] * qrow[1] + prow[2] * qrow[2]
    half = 0.5 * (a_val - c_val)
    disc = half * half + b_val * b_val + 0.01
    return 0.5 * (a_val + c_val) + disc * lax.rsqrt(disc)


Y, Z = 4, 8


def near(step):
    y, z = (min(a, n - a) for a, n in zip(step, (Y, Z)))
    return y + z, z


STEPS = sorted(((a, b) for a in range(Y) for b in range(Z)), key=near)
YO, ZO = zip(*STEPS)
GROUPS = (5, 7, 8, 7, 5)
LAG = (2, 4)
SETTLE = 1


def pick(table, index):
    out = jnp.full(index.shape, table[0], jnp.int32)
    for i in range(1, len(table)):
        out = jnp.where(index == i, table[i], out)
    return out


def main_kernel(
    V, S, views, rots_h, trns_h, foc_h, mask_h, means_h, scales_h, quats_h, attrs_h, grad_h, vis_h,
    buf, peak, where_out,
    rots, trns, foc, mask, means, scales, quats, grad, vis, fac, x, enc, g, split, packed, send, found_v, cnt, counts,
    local, halves, merged, whole, lsem, csend, crecv, psend, precv,
    fsend, frecv, xsend, xrecv, hsend, hrecv, msend, mrecv,
):
    v, s = lax.axis_index("view"), lax.axis_index("gauss")
    nblk = mask.shape[0]
    per = nblk // S
    X = V // 2
    core = lax.rem(v, 2)
    chip = lax.div(v, 2)
    mate = v + 1 - 2 * core
    nxt = 2 * lax.rem(chip + 1, X) + core
    prv = 2 * lax.rem(chip + X - 1, X) + core
    opp = 2 * lax.rem(chip + 2, X) + core
    y, z = lax.div(s, Z), lax.rem(s, Z)
    i32, f32, bf16 = jnp.int32, jnp.float32, jnp.bfloat16

    def dest(p):
        return lax.rem(y + YO[p], Y) * Z + lax.rem(z + ZO[p], Z)

    bar = pltpu.get_barrier_semaphore()
    for p in range(1, S):
        pl.semaphore_signal(bar, inc=1, device_id=peer(v, dest(p)), device_id_type=MESH)
    for to in (mate, nxt, prv, opp):
        pl.semaphore_signal(bar, inc=1, device_id=peer(to, s), device_id_type=MESH)

    @pl.when(v == V - 1)
    def _():
        for k in range(X - 1):
            pl.semaphore_signal(bar, inc=1, device_id=peer(2 * k, s), device_id_type=MESH)

    loads = [
        pltpu.make_async_copy(a, b, lsem.at[i])
        for i, (a, b) in enumerate((
            (mask_h, mask), (means_h, means), (scales_h, scales), (quats_h, quats),
            (grad_h, grad), (vis_h, vis), (rots_h, rots), (trns_h, trns), (foc_h, foc),
        ))
    ]
    for c in loads:
        c.start()

    def tiles(act):
        for t in range(1, TILES):
            @pl.when(v == t)
            def _():
                n = 6 if t < TILES - 1 else 1
                act(pltpu.make_async_copy(
                    attrs_h.at[pl.ds((t - 1) * SUB, n), :], x.at[pl.ds(0, n), :], lsem.at[9]
                ))
                if t > 1:
                    act(pltpu.make_async_copy(
                        attrs_h.at[pl.ds((t - 2) * SUB + 6, 2), :], x.at[pl.ds(6, 2), :], lsem.at[10]
                    ))

    loads[0].wait()
    m = mask[...]
    cnt[...] = jnp.full((1, LANES), jnp.sum(m), i32)
    step = 2 * SUB

    def lines(ref, i, count, c):
        return ref[pl.ds(i * step * count + c, step, stride=count), :]

    for i in (1, 2, 3):
        loads[i].wait()

    def shape(i, carry):
        rows = pl.ds(pl.multiple_of(i * step, step), step)
        factor = quat_factor(
            [scales[rows, c, :] for c in range(3)], [lines(quats, i, 4, c) for c in range(4)]
        )
        for c in range(3):
            fac[9 + c, rows, :] = means[rows, c, :]
            for e in range(3):
                fac[3 * c + e, rows, :] = factor[c][e]
        return carry

    lax.fori_loop(0, nblk // step, shape, 0)
    for i in range(4, 9):
        loads[i].wait()
    tiles(lambda c: c.start())
    for u in range(views):
        rot = [[rots[a, u, b] for b in range(3)] for a in range(3)]
        trans = [trns[u, a] for a in range(3)]
        fl = foc[u]

        def look(i, carry):
            rows = pl.ds(pl.multiple_of(i * step, step), step)
            factor = [[fac[3 * a + b, rows, :] for b in range(3)] for a in range(3)]
            lam = view_lam([fac[9 + c, rows, :] for c in range(3)], factor, rot, trans, fl)
            seen = lines(vis, i, views, u) != 0
            g0, g1 = (grad[u, pl.ds(i * step * 2 + c, step, stride=2), :] for c in range(2))
            for c, value in enumerate((g0 * g0 + g1 * g1, lam)):
                at = pl.ds(i * step * 2 + c, step, stride=2)
                value = jnp.where(seen, value, 0.0)
                local[at, :] = value if u == 0 else jnp.maximum(local[at, :], value)
            return carry

        lax.fori_loop(0, nblk // step, look, 0)

    started = []

    def remote(a, b, ss, rs, to):
        return pltpu.make_async_remote_copy(
            src_ref=a, dst_ref=b, send_sem=ss, recv_sem=rs, device_id=to, device_id_type=MESH
        )

    def go(copy):
        copy.start()
        started.append(copy)
        return copy

    pl.semaphore_wait(bar, S + 3 + jnp.where((core == 0) & (chip < X - 1), 1, 0))
    tally = [
        go(remote(cnt, counts.at[pl.ds(p, 1), :], csend.at[p], crecv.at[p], peer(v, dest(p))))
        for p in reversed(range(1, S))
    ]
    mine = pl.ds(pl.multiple_of(core * nblk, nblk), nblk)
    last = V - 1
    pair = go(remote(local, halves, psend.at[0], precv.at[0], peer(mate, s)))
    counts[0:1, :] = cnt[...]

    lane = lax.broadcasted_iota(i32, (nblk, LANES), 1)
    row = lax.broadcasted_iota(i32, (nblk, LANES), 0)
    mb = m.astype(bf16)
    before = (row < lane).astype(bf16)
    above = (row > lane).astype(bf16)
    dot = functools.partial(jnp.dot, preferred_element_type=f32)
    ones = jnp.ones((LANES, LANES), bf16)
    rank = dot(mb, before).astype(i32)
    size = dot(mb, ones).astype(i32)
    base = dot(dot(above, mb).astype(bf16), ones).astype(i32)
    flat = lax.dot_general(
        jnp.ones((SUB, LANES), bf16), mb, (((1,), (1,)), ((), ())), preferred_element_type=f32
    )
    starts = dot(flat.astype(bf16), before).astype(i32)
    code = jnp.where(m == 1, 65536 + (lane - rank) * 256 + lane, 0)
    bit = 1
    while bit < LANES:
        moved = pltpu.roll(code, LANES - bit, 1)
        goes = (moved & (bit * 256)) != 0
        stays = (code & (bit * 256)) == 0
        code = jnp.where(goes, moved, jnp.where(stays, code, 0))
        bit *= 2
    turn = (lane - base) & (LANES - 1)
    src = jnp.take_along_axis(code & (LANES - 1), turn, axis=1)
    valid = turn < size
    idx = jnp.where(valid, src, 0)
    enc[...] = jnp.where(valid, src, -1)
    head = lane >= (base & (LANES - 1))
    low, high = valid & head, valid & jnp.logical_not(head)


    pair.wait_recv()
    merged[...] = jnp.maximum(local[...], halves[...])
    spread = []
    for k in range(1, X):
        to = lax.rem(chip + k, X)
        spread.append(go(remote(
            merged.at[mine, :], whole.at[k - 1, mine, :], psend.at[k], precv.at[k + X * core],
            peer(2 * to + jnp.where(to == X - 1, 1, core), s),
        )))

    tiles(lambda c: c.wait())

    @pl.when(v > 0)
    def _():
        def gather(b, carry):
            e = jnp.broadcast_to(enc[pl.ds(b, 1), :], (SUB, LANES))
            cols = pl.ds(pl.multiple_of(b * LANES, LANES), LANES)
            got = jnp.take_along_axis(x[:, cols], jnp.maximum(e, 0), axis=1)
            g[b] = got
            return carry

        lax.fori_loop(0, nblk, gather, 0, unroll=8)

    def put(final, value):
        g[:, (final + 6) % SUB, :] = jnp.take_along_axis(value, idx, axis=1)

    @pl.when(v == 0)
    def _():
        for c in range(3):
            put(c, means[:, c, :])
            put(3 + c, scales[:, c, :])
        for c in range(2):
            put(6 + c, quats[pl.ds(c, nblk, stride=4), :])

    @pl.when(v == 1)
    def _():
        for c in range(2):
            put(c, quats[pl.ds(2 + c, nblk, stride=4), :])

    def cut(c):
        value = g[:, (c + 6) % SUB, :]
        for part, keep in enumerate((low, high)):
            rest = jnp.where(keep, value, 0.0)
            for i in range(3):
                top = rest.astype(bf16)
                split[(2 * i + part) * nblk:(2 * i + part + 1) * nblk, c * LANES:(c + 1) * LANES] = top
                rest = rest - top.astype(f32)

    at = starts[0:1, :] >> 7
    hot = jnp.concatenate([(row == at).astype(bf16), (row == at + 1).astype(bf16)] * 3, axis=1)

    def pack(*finals):
        for c in finals:
            cut(c)
        lo, hi = finals[0], finals[-1] + 1
        moved = dot(hot, split[:, lo * LANES:hi * LANES])
        for c in finals:
            packed[:, c, :] = moved[:, (c - lo) * LANES:(c - lo + 1) * LANES]

    full = remote(peak.at[mine, :], peak.at[mine, :], psend.at[X + 1], precv.at[X], peer(mate, s))
    extra = remote(peak, peak, psend.at[X], precv.at[X], peer(mate, s))

    def arrive(half):
        for k in range(1, X):
            ref = whole.at[k - 1, pl.ds(half * nblk, nblk), :]
            remote(ref, ref, psend.at[k], precv.at[k + X * half], peer(mate, s)).wait_recv()

    def finish(rows):
        best = merged[rows, :]
        for k in range(X - 1):
            best = jnp.maximum(best, whole[k, rows, :])
        odd = (lax.broadcasted_iota(i32, best.shape, 0) & 1) == 1
        peak[rows, :] = jnp.sqrt(best) * jnp.where(odd, 3.0, 1.0)

    pack(0, 1, 2)

    @pl.when(v < TILES - 1)
    def _():
        pack(3, 4, 5, 6, 7)

    @pl.when(v == TILES - 1)
    def _():
        packed[:, 5:, :] = jnp.zeros((nblk, 3, LANES), f32)
        arrive(0)
        arrive(1)
        finish(pl.ds(0, 2 * nblk))
        extra.start()
        for c in range(2):
            put(3 + c, peak[pl.ds(c, nblk, stride=2), :])
        pack(3, 4)

    def source(p):
        return ((y - pick(YO, p)) & (Y - 1)) * Z + ((z - pick(ZO, p)) & (Z - 1))

    p32 = lax.broadcasted_iota(i32, (S, LANES), 0)
    lower = source(p32) < s
    for c in tally:
        c.wait_recv()
    tot = counts[...]
    blocks = (tot + (LANES - 1)) >> 7
    offset = jnp.sum(jnp.where(lower, blocks, 0), axis=0)[0]
    for p in range(S):
        first = (dest(p) - offset) & (S - 1)
        for w in range(per):
            send[p * per + w] = packed[first + S * w]

    fars = [None]
    for p in range(1, S):
        fars.append(go(remote(
            send.at[pl.ds(p * per, per)], buf.at[v, pl.ds(p * per, per)],
            fsend.at[p], frecv.at[p], peer(v, dest(p)),
        )))
    own = pltpu.make_async_copy(send.at[pl.ds(0, per)], buf.at[v, pl.ds(0, per)], fsend.at[0])
    own.start()

    def settle():
        for half in range(2):
            @pl.when((chip < X - 1) & (core == half))
            def _():
                arrive(half)
                finish(mine)
                full.start()

    pr = lax.broadcasted_iota(i32, (S, S), 0)
    pc = lax.broadcasted_iota(i32, (S, S), 1)
    less = (source(pc) < source(pr)).astype(bf16)
    offs = dot(less, blocks.astype(bf16)).astype(i32)
    k = lax.broadcasted_iota(i32, (S, LANES), 1) * S + s
    here = (k >= offs) & (k < offs + blocks)
    spot = jnp.where(here, p32 * per + ((k - offs) >> 5) + 1, 0)
    found = jnp.sum(spot, axis=0, keepdims=True) - 1
    total = jnp.sum(tot, axis=0, keepdims=True)
    sub = lax.broadcasted_iota(i32, (SUB, LANES), 0)
    found_v[...] = jnp.where(sub == 0, found, total)
    tell = pltpu.make_async_copy(found_v, where_out, lsem.at[0])
    tell.start()

    edges = [0]
    for n in GROUPS:
        edges.append(edges[-1] + n)
    N = len(GROUPS)

    def group(owner, i, half=None):
        first, size = edges[i] * per, GROUPS[i] * per
        if half is not None:
            size //= 2
            first += half * size
        return buf.at[owner, pl.ds(first, size)]

    def ring(i, way):
        return remote(group(v, i), group(v, i), xsend.at[way, i], xrecv.at[way, i], peer((nxt, prv)[way], s))

    def relay(i, way):
        ref = group((prv, nxt)[way], i, way)
        return remote(ref, ref, hsend.at[way, i], hrecv.at[way, i], peer((nxt, prv)[way], s))

    def beside(i, q):
        ref = group((v, prv, nxt, opp)[q], i)
        return remote(ref, ref, msend.at[q, i], mrecv.at[q, i], peer(mate, s))

    rings, relays, besides = {}, {}, {}
    for i in range(N + LAG[1]):
        if i < N:
            for p in range(edges[i], edges[i + 1]):
                if p:
                    fars[p].wait_recv()
                else:
                    own.wait()
            for way in range(2):
                rings[i, way] = go(ring(i, way))
            besides[i, 0] = go(beside(i, 0))
        if i == SETTLE:
            settle()
        j = i - LAG[0]
        if 0 <= j < N:
            for way in range(2):
                rings[j, way].wait_recv()
                relays[j, way] = go(relay(j, way))
            for way in range(2):
                besides[j, 1 + way] = go(beside(j, 1 + way))
        j = i - LAG[1]
        if 0 <= j < N:
            for way in range(2):
                relays[j, way].wait_recv()
            besides[j, 3] = go(beside(j, 3))
    @pl.when(chip < X - 1)
    def _():
        full.wait()

    @pl.when(v == last - 1)
    def _():
        extra.wait_recv()

    @pl.when(v == last)
    def _():
        extra.wait_send()

    tell.wait()
    for c in besides.values():
        c.wait_recv()
    for c in started:
        c.wait_send()


def place_kernel(idx, peak_in, buf, clones, peak, total, out, osem, psem):
    rows = clones.shape[0]
    slots = out.shape[1] // LANES
    chunks = osem.shape[0]
    top = pltpu.make_async_copy(peak_in, peak, psem)
    top.start()
    total[0] = idx[1, 0]
    each = slots // chunks
    outs = []
    for c in range(chunks):
        def one(q, carry):
            r = idx[0, q]
            on = r >= 0
            r = jnp.maximum(r, 0)
            cols = pl.ds(pl.multiple_of(q * LANES, LANES), LANES)
            for i in range(TILES):
                n = min(rows - i * SUB, SUB)
                out[i * SUB:i * SUB + n, cols] = jnp.where(on, buf[i, r], 0.0)[:n]
            return carry

        lax.fori_loop(c * each, (c + 1) * each, one, 0, unroll=4)
        cols = pl.ds(c * each * LANES, each * LANES)
        cp = pltpu.make_async_copy(out.at[:, cols], clones.at[:, cols], osem.at[c])
        cp.start()
        outs.append(cp)
    for cp in outs:
        cp.wait()
    top.wait()


def body(V, S, means, scales, quats, attrs, grad_screen, visible, clone_mask, rotation, shift, focal):
    G = clone_mask.shape[0]
    nblk = G // LANES
    views = grad_screen.shape[0]
    rows = means.shape[0] + scales.shape[0] + quats.shape[0] + attrs.shape[0] + 2
    f32, i32 = jnp.float32, jnp.int32

    def lines(a):
        a = a.reshape(a.shape[:-1] + (nblk, LANES))
        return jnp.swapaxes(a, -3, -2)

    dma = pltpu.SemaphoreType.DMA
    N = len(GROUPS)
    limit = 32 * 1024 * 1024
    buf, peak, where = pl.pallas_call(
        functools.partial(main_kernel, V, S, views),
        out_shape=(
            VMEM((V, nblk, SUB, LANES), f32), VMEM((2 * nblk, LANES), f32), SMEM((SUB, LANES), i32),
        ),
        in_specs=[spec(HBM)] * 10,
        out_specs=(spec(VMEM), spec(VMEM), spec(SMEM)),
        scratch_shapes=[
            SMEM((3, views, 3), f32),
            SMEM((views, 3), f32),
            SMEM((views,), f32),
            VMEM((nblk, LANES), i32),
            VMEM((nblk, 3, LANES), f32),
            VMEM((nblk, 3, LANES), f32),
            VMEM((4 * nblk, LANES), f32),
            VMEM((views, 2 * nblk, LANES), f32),
            VMEM((views * nblk, LANES), i32),
            VMEM((12, nblk, LANES), f32),
            VMEM((SUB, G), f32),
            VMEM((nblk, LANES), i32),
            VMEM((nblk, SUB, LANES), f32),
            VMEM((6 * nblk, SUB * LANES), jnp.bfloat16),
            VMEM((nblk, SUB, LANES), f32),
            VMEM((nblk, SUB, LANES), f32),
            VMEM((SUB, LANES), i32),
            VMEM((1, LANES), i32),
            VMEM((S, LANES), i32),
            VMEM((2 * nblk, LANES), f32),
            VMEM((2 * nblk, LANES), f32),
            VMEM((2 * nblk, LANES), f32),
            VMEM((V // 2 - 1, 2 * nblk, LANES), f32),
            dma((11,)), dma((S,)), dma((S,)), dma((V,)), dma((V,)),
            dma((S,)), dma((S,)), dma((2, N)), dma((2, N)), dma((2, N)), dma((2, N)),
            dma((4, N)), dma((4, N)),
        ],
        compiler_params=pltpu.CompilerParams(
            collective_id=0, has_side_effects=True, vmem_limit_bytes=limit
        ),
        name="main",
    )(*(
        pltpu.with_memory_space_constraint(a, HBM)
        for a in (
            jnp.transpose(rotation, (1, 0, 2)), shift, focal, clone_mask.reshape(nblk, LANES),
            lines(means), lines(scales), lines(quats).reshape(-1, LANES), attrs,
            lines(grad_screen).reshape(views, -1, LANES), lines(visible).reshape(-1, LANES),
        )
    ))
    chunks = 8
    clones, peak, total = pl.pallas_call(
        place_kernel,
        out_shape=(
            jax.ShapeDtypeStruct((rows, G), f32),
            jax.ShapeDtypeStruct((2 * nblk, LANES), f32),
            jax.ShapeDtypeStruct((1,), i32),
        ),
        in_specs=[spec(SMEM), spec(VMEM), spec(VMEM)],
        out_specs=(spec(pl.ANY), spec(pl.ANY), spec(SMEM)),
        scratch_shapes=[VMEM((rows, G), f32), dma((chunks,)), dma],
        compiler_params=pltpu.CompilerParams(vmem_limit_bytes=limit),
        name="place",
    )(where, peak, buf)
    peak = jnp.swapaxes(peak.reshape(nblk, 2, LANES), 0, 1).reshape(2, G)
    return peak, clones, total.reshape(())


def solution(mesh):
    return jax.shard_map(
        functools.partial(body, mesh.shape["view"], mesh.shape["gauss"]),
        mesh=mesh,
        in_specs=(
            P(None, "gauss"),
            P(None, "gauss"),
            P(None, "gauss"),
            P(None, "gauss"),
            P("view", None, "gauss"),
            P("view", "gauss"),
            P("gauss"),
            P("view", None, None),
            P("view", None),
            P("view"),
        ),
        out_specs=(P(None, "gauss"), P(None, "gauss"), P()),
        check_vma=False,
    )
```

```python
import functools

import jax
import jax.numpy as jnp
from jax import lax
from jax.experimental import pallas as pl
from jax.experimental.pallas import tpu as pltpu
from jax.sharding import PartitionSpec as P

LANES = 128
SUB = 8
TILES = 8
VMEM = pltpu.VMEM
SMEM = pltpu.SMEM
HBM = pltpu.HBM
MESH = pl.DeviceIdType.MESH


def spec(space):
    return pl.BlockSpec(memory_space=space)


def peer(view, gauss):
    return {"view": view, "gauss": gauss}


def quat_factor(scales, quats):
    w, x, y, z = quats
    inv = lax.rsqrt(w * w + x * x + y * y + z * z + 0.25)
    w, x, y, z = (w * inv, x * inv, y * inv, z * inv)
    rq = [
        [1 - 2 * (y * y + z * z), 2 * (x * y - w * z), 2 * (x * z + w * y)],
        [2 * (x * y + w * z), 1 - 2 * (x * x + z * z), 2 * (y * z - w * x)],
        [2 * (x * z - w * y), 2 * (y * z + w * x), 1 - 2 * (x * x + y * y)],
    ]
    return [[rq[i][j] * scales[j] for j in range(3)] for i in range(3)]


def view_lam(means, factor, rot, trans, focal_v):
    point = [
        rot[i][0] * means[0] + rot[i][1] * means[1] + rot[i][2] * means[2] + trans[i]
        for i in range(3)
    ]
    inv = 1.0 / jnp.maximum(point[2], 1.0)
    j00 = focal_v * inv
    j02 = -(j00 * point[0]) * inv
    j12 = -(j00 * point[1]) * inv
    first = [j00 * rot[0][j] + j02 * rot[2][j] for j in range(3)]
    second = [j00 * rot[1][j] + j12 * rot[2][j] for j in range(3)]
    prow = [sum((first[j] * factor[j][k] for j in range(3))) for k in range(3)]
    qrow = [sum((second[j] * factor[j][k] for j in range(3))) for k in range(3)]
    a_val = prow[0] * prow[0] + prow[1] * prow[1] + prow[2] * prow[2] + 0.3
    c_val = qrow[0] * qrow[0] + qrow[1] * qrow[1] + qrow[2] * qrow[2] + 0.3
    b_val = prow[0] * qrow[0] + prow[1] * qrow[1] + prow[2] * qrow[2]
    half = 0.5 * (a_val - c_val)
    disc = half * half + b_val * b_val + 0.01
    return 0.5 * (a_val + c_val) + disc * lax.rsqrt(disc)


Y, Z = 4, 8


def near(step):
    y, z = (min(a, n - a) for a, n in zip(step, (Y, Z)))
    return y + z, z


STEPS = sorted(((a, b) for a in range(Y) for b in range(Z)), key=near)
YO, ZO = zip(*STEPS)
GROUPS = (5, 7, 8, 7, 5)
LAG = (2, 4)
SETTLE = 1


def pick(table, index):
    out = jnp.full(index.shape, table[0], jnp.int32)
    for i in range(1, len(table)):
        out = jnp.where(index == i, table[i], out)
    return out


def main_kernel(
    V, S, views, rots_h, trns_h, foc_h, mask_h, means_h, scales_h, quats_h, attrs_h, grad_h, vis_h,
    buf, peak, where_out,
    rots, trns, foc, mask, means, scales, quats, grad, vis, fac, x, enc, g, split, packed, send, found_v, cnt, counts,
    local, halves, merged, whole, lsem, csend, crecv, psend, precv,
    fsend, frecv, xsend, xrecv, hsend, hrecv, msend, mrecv,
):
    v, s = lax.axis_index("view"), lax.axis_index("gauss")
    nblk = mask.shape[0]
    per = nblk // S
    X = V // 2
    core = lax.rem(v, 2)
    chip = lax.div(v, 2)
    mate = v + 1 - 2 * core
    nxt = 2 * lax.rem(chip + 1, X) + core
    prv = 2 * lax.rem(chip + X - 1, X) + core
    opp = 2 * lax.rem(chip + 2, X) + core
    y, z = lax.div(s, Z), lax.rem(s, Z)
    i32, f32, bf16 = jnp.int32, jnp.float32, jnp.bfloat16

    def dest(p):
        return lax.rem(y + YO[p], Y) * Z + lax.rem(z + ZO[p], Z)

    bar = pltpu.get_barrier_semaphore()
    for p in range(1, S):
        pl.semaphore_signal(bar, inc=1, device_id=peer(v, dest(p)), device_id_type=MESH)
    for to in (mate, nxt, prv, opp):
        pl.semaphore_signal(bar, inc=1, device_id=peer(to, s), device_id_type=MESH)

    @pl.when(v == V - 1)
    def _():
        for k in range(X - 1):
            pl.semaphore_signal(bar, inc=1, device_id=peer(2 * k, s), device_id_type=MESH)

    loads = [
        pltpu.make_async_copy(a, b, lsem.at[i])
        for i, (a, b) in enumerate((
            (mask_h, mask), (means_h, means), (scales_h, scales), (quats_h, quats),
            (grad_h, grad), (vis_h, vis), (rots_h, rots), (trns_h, trns), (foc_h, foc),
        ))
    ]
    for c in loads:
        c.start()

    def tiles(act):
        for t in range(1, TILES):
            @pl.when(v == t)
            def _():
                n = 6 if t < TILES - 1 else 1
                act(pltpu.make_async_copy(
                    attrs_h.at[pl.ds((t - 1) * SUB, n), :], x.at[pl.ds(0, n), :], lsem.at[9]
                ))
                if t > 1:
                    act(pltpu.make_async_copy(
                        attrs_h.at[pl.ds((t - 2) * SUB + 6, 2), :], x.at[pl.ds(6, 2), :], lsem.at[10]
                    ))

    loads[0].wait()
    m = mask[...]
    cnt[...] = jnp.full((1, LANES), jnp.sum(m), i32)
    step = 2 * SUB

    def lines(ref, i, count, c):
        return ref[pl.ds(i * step * count + c, step, stride=count), :]

    for i in (1, 2, 3):
        loads[i].wait()

    def shape(i, carry):
        rows = pl.ds(pl.multiple_of(i * step, step), step)
        factor = quat_factor(
            [scales[rows, c, :] for c in range(3)], [lines(quats, i, 4, c) for c in range(4)]
        )
        for c in range(3):
            fac[9 + c, rows, :] = means[rows, c, :]
            for e in range(3):
                fac[3 * c + e, rows, :] = factor[c][e]
        return carry

    lax.fori_loop(0, nblk // step, shape, 0)
    for i in range(4, 9):
        loads[i].wait()
    tiles(lambda c: c.start())
    for u in range(views):
        rot = [[rots[a, u, b] for b in range(3)] for a in range(3)]
        trans = [trns[u, a] for a in range(3)]
        fl = foc[u]

        def look(i, carry):
            rows = pl.ds(pl.multiple_of(i * step, step), step)
            factor = [[fac[3 * a + b, rows, :] for b in range(3)] for a in range(3)]
            lam = view_lam([fac[9 + c, rows, :] for c in range(3)], factor, rot, trans, fl)
            seen = lines(vis, i, views, u) != 0
            g0, g1 = (grad[u, pl.ds(i * step * 2 + c, step, stride=2), :] for c in range(2))
            for c, value in enumerate((g0 * g0 + g1 * g1, lam)):
                at = pl.ds(i * step * 2 + c, step, stride=2)
                value = jnp.where(seen, value, 0.0)
                local[at, :] = value if u == 0 else jnp.maximum(local[at, :], value)
            return carry

        lax.fori_loop(0, nblk // step, look, 0)

    started = []

    def remote(a, b, ss, rs, to):
        return pltpu.make_async_remote_copy(
            src_ref=a, dst_ref=b, send_sem=ss, recv_sem=rs, device_id=to, device_id_type=MESH
        )

    def go(copy):
        copy.start()
        started.append(copy)
        return copy

    pl.semaphore_wait(bar, S + 3 + jnp.where((core == 0) & (chip < X - 1), 1, 0))
    tally = [
        go(remote(cnt, counts.at[pl.ds(p, 1), :], csend.at[p], crecv.at[p], peer(v, dest(p))))
        for p in reversed(range(1, S))
    ]
    mine = pl.ds(pl.multiple_of(core * nblk, nblk), nblk)
    last = V - 1
    pair = go(remote(local, halves, psend.at[0], precv.at[0], peer(mate, s)))
    counts[0:1, :] = cnt[...]

    lane = lax.broadcasted_iota(i32, (nblk, LANES), 1)
    row = lax.broadcasted_iota(i32, (nblk, LANES), 0)
    mb = m.astype(bf16)
    before = (row < lane).astype(bf16)
    above = (row > lane).astype(bf16)
    dot = functools.partial(jnp.dot, preferred_element_type=f32)
    ones = jnp.ones((LANES, LANES), bf16)
    rank = dot(mb, before).astype(i32)
    size = dot(mb, ones).astype(i32)
    base = dot(dot(above, mb).astype(bf16), ones).astype(i32)
    flat = lax.dot_general(
        jnp.ones((SUB, LANES), bf16), mb, (((1,), (1,)), ((), ())), preferred_element_type=f32
    )
    starts = dot(flat.astype(bf16), before).astype(i32)
    code = jnp.where(m == 1, 65536 + (lane - rank) * 256 + lane, 0)
    bit = 1
    while bit < LANES:
        moved = pltpu.roll(code, LANES - bit, 1)
        goes = (moved & (bit * 256)) != 0
        stays = (code & (bit * 256)) == 0
        code = jnp.where(goes, moved, jnp.where(stays, code, 0))
        bit *= 2
    turn = (lane - base) & (LANES - 1)
    src = jnp.take_along_axis(code & (LANES - 1), turn, axis=1)
    valid = turn < size
    idx = jnp.where(valid, src, 0)
    enc[...] = jnp.where(valid, src, -1)
    head = lane >= (base & (LANES - 1))
    low, high = valid & head, valid & jnp.logical_not(head)


    pair.wait_recv()
    merged[...] = jnp.maximum(local[...], halves[...])
    spread = []
    for k in range(1, X):
        to = lax.rem(chip + k, X)
        spread.append(go(remote(
            merged.at[mine, :], whole.at[k - 1, mine, :], psend.at[k], precv.at[k + X * core],
            peer(2 * to + jnp.where(to == X - 1, 1, core), s),
        )))

    tiles(lambda c: c.wait())

    @pl.when(v > 0)
    def _():
        def gather(b, carry):
            e = jnp.broadcast_to(enc[pl.ds(b, 1), :], (SUB, LANES))
            cols = pl.ds(pl.multiple_of(b * LANES, LANES), LANES)
            got = jnp.take_along_axis(x[:, cols], jnp.maximum(e, 0), axis=1)
            g[b] = got
            return carry

        lax.fori_loop(0, nblk, gather, 0, unroll=8)

    def put(final, value):
        g[:, (final + 6) % SUB, :] = jnp.take_along_axis(value, idx, axis=1)

    @pl.when(v == 0)
    def _():
        for c in range(3):
            put(c, means[:, c, :])
            put(3 + c, scales[:, c, :])
        for c in range(2):
            put(6 + c, quats[pl.ds(c, nblk, stride=4), :])

    @pl.when(v == 1)
    def _():
        for c in range(2):
            put(c, quats[pl.ds(2 + c, nblk, stride=4), :])

    def cut(c):
        value = g[:, (c + 6) % SUB, :]
        for part, keep in enumerate((low, high)):
            rest = jnp.where(keep, value, 0.0)
            for i in range(3):
                top = rest.astype(bf16)
                split[(2 * i + part) * nblk:(2 * i + part + 1) * nblk, c * LANES:(c + 1) * LANES] = top
                rest = rest - top.astype(f32)

    at = starts[0:1, :] >> 7
    hot = jnp.concatenate([(row == at).astype(bf16), (row == at + 1).astype(bf16)] * 3, axis=1)

    def pack(*finals):
        for c in finals:
            cut(c)
        lo, hi = finals[0], finals[-1] + 1
        moved = dot(hot, split[:, lo * LANES:hi * LANES])
        for c in finals:
            packed[:, c, :] = moved[:, (c - lo) * LANES:(c - lo + 1) * LANES]

    full = remote(peak.at[mine, :], peak.at[mine, :], psend.at[X + 1], precv.at[X], peer(mate, s))
    extra = remote(peak, peak, psend.at[X], precv.at[X], peer(mate, s))

    def arrive(half):
        for k in range(1, X):
            ref = whole.at[k - 1, pl.ds(half * nblk, nblk), :]
            remote(ref, ref, psend.at[k], precv.at[k + X * half], peer(mate, s)).wait_recv()

    def finish(rows):
        best = merged[rows, :]
        for k in range(X - 1):
            best = jnp.maximum(best, whole[k, rows, :])
        odd = (lax.broadcasted_iota(i32, best.shape, 0) & 1) == 1
        peak[rows, :] = jnp.sqrt(best) * jnp.where(odd, 3.0, 1.0)

    pack(0, 1, 2)

    @pl.when(v < TILES - 1)
    def _():
        pack(3, 4, 5, 6, 7)

    @pl.when(v == TILES - 1)
    def _():
        packed[:, 5:, :] = jnp.zeros((nblk, 3, LANES), f32)
        arrive(0)
        arrive(1)
        finish(pl.ds(0, 2 * nblk))
        extra.start()
        for c in range(2):
            put(3 + c, peak[pl.ds(c, nblk, stride=2), :])
        pack(3, 4)

    def source(p):
        return ((y - pick(YO, p)) & (Y - 1)) * Z + ((z - pick(ZO, p)) & (Z - 1))

    p32 = lax.broadcasted_iota(i32, (S, LANES), 0)
    lower = source(p32) < s
    for c in tally:
        c.wait_recv()
    tot = counts[...]
    blocks = (tot + (LANES - 1)) >> 7
    offset = jnp.sum(jnp.where(lower, blocks, 0), axis=0)[0]
    for p in range(S):
        first = (dest(p) - offset) & (S - 1)
        for w in range(per):
            send[p * per + w] = packed[first + S * w]

    fars = [None]
    for p in range(1, S):
        fars.append(go(remote(
            send.at[pl.ds(p * per, per)], buf.at[v, pl.ds(p * per, per)],
            fsend.at[p], frecv.at[p], peer(v, dest(p)),
        )))
    own = pltpu.make_async_copy(send.at[pl.ds(0, per)], buf.at[v, pl.ds(0, per)], fsend.at[0])
    own.start()

    def settle():
        for half in range(2):
            @pl.when((chip < X - 1) & (core == half))
            def _():
                arrive(half)
                finish(mine)
                full.start()

    pr = lax.broadcasted_iota(i32, (S, S), 0)
    pc = lax.broadcasted_iota(i32, (S, S), 1)
    less = (source(pc) < source(pr)).astype(bf16)
    offs = dot(less, blocks.astype(bf16)).astype(i32)
    k = lax.broadcasted_iota(i32, (S, LANES), 1) * S + s
    here = (k >= offs) & (k < offs + blocks)
    spot = jnp.where(here, p32 * per + ((k - offs) >> 5) + 1, 0)
    found = jnp.sum(spot, axis=0, keepdims=True) - 1
    total = jnp.sum(tot, axis=0, keepdims=True)
    sub = lax.broadcasted_iota(i32, (SUB, LANES), 0)
    found_v[...] = jnp.where(sub == 0, found, total)
    tell = pltpu.make_async_copy(found_v, where_out, lsem.at[0])
    tell.start()

    edges = [0]
    for n in GROUPS:
        edges.append(edges[-1] + n)
    N = len(GROUPS)

    def group(owner, i, half=None):
        first, size = edges[i] * per, GROUPS[i] * per
        if half is not None:
            size //= 2
            first += half * size
        return buf.at[owner, pl.ds(first, size)]

    def ring(i, way):
        return remote(group(v, i), group(v, i), xsend.at[way, i], xrecv.at[way, i], peer((nxt, prv)[way], s))

    def relay(i, way):
        ref = group((prv, nxt)[way], i, way)
        return remote(ref, ref, hsend.at[way, i], hrecv.at[way, i], peer((nxt, prv)[way], s))

    def beside(i, q):
        ref = group((v, prv, nxt, opp)[q], i)
        return remote(ref, ref, msend.at[q, i], mrecv.at[q, i], peer(mate, s))

    rings, relays, besides = {}, {}, {}
    done = set()
    marks = {N - 1: len(started)}
    for i in range(N + LAG[1]):
        if i < N:
            for p in range(edges[i], edges[i + 1]):
                if p:
                    fars[p].wait_recv()
                else:
                    own.wait()
            for way in range(2):
                rings[i, way] = go(ring(i, way))
            besides[i, 0] = go(beside(i, 0))
        if i == SETTLE:
            settle()
        for c in started[:marks.get(i, 0)]:
            c.wait_send()
            done.add(id(c))
        j = i - LAG[0]
        if 0 <= j < N:
            for way in range(2):
                rings[j, way].wait_recv()
                relays[j, way] = go(relay(j, way))
            for way in range(2):
                besides[j, 1 + way] = go(beside(j, 1 + way))
        j = i - LAG[1]
        if 0 <= j < N:
            for way in range(2):
                relays[j, way].wait_recv()
            besides[j, 3] = go(beside(j, 3))
    @pl.when(chip < X - 1)
    def _():
        full.wait()

    @pl.when(v == last - 1)
    def _():
        extra.wait_recv()

    @pl.when(v == last)
    def _():
        extra.wait_send()

    tell.wait()
    for c in besides.values():
        c.wait_recv()
    for c in started:
        if id(c) not in done:
            c.wait_send()


def place_kernel(idx, peak_in, buf, clones, peak, total, out, osem, psem):
    rows = clones.shape[0]
    slots = out.shape[1] // LANES
    chunks = osem.shape[0]
    top = pltpu.make_async_copy(peak_in, peak, psem)
    top.start()
    total[0] = idx[1, 0]
    each = slots // chunks
    outs = []
    for c in range(chunks):
        def one(q, carry):
            r = idx[0, q]
            on = r >= 0
            r = jnp.maximum(r, 0)
            cols = pl.ds(pl.multiple_of(q * LANES, LANES), LANES)
            for i in range(TILES):
                n = min(rows - i * SUB, SUB)
                out[i * SUB:i * SUB + n, cols] = jnp.where(on, buf[i, r], 0.0)[:n]
            return carry

        lax.fori_loop(c * each, (c + 1) * each, one, 0, unroll=4)
        cols = pl.ds(c * each * LANES, each * LANES)
        cp = pltpu.make_async_copy(out.at[:, cols], clones.at[:, cols], osem.at[c])
        cp.start()
        outs.append(cp)
    for cp in outs:
        cp.wait()
    top.wait()


def body(V, S, means, scales, quats, attrs, grad_screen, visible, clone_mask, rotation, shift, focal):
    G = clone_mask.shape[0]
    nblk = G // LANES
    views = grad_screen.shape[0]
    rows = means.shape[0] + scales.shape[0] + quats.shape[0] + attrs.shape[0] + 2
    f32, i32 = jnp.float32, jnp.int32

    def lines(a):
        a = a.reshape(a.shape[:-1] + (nblk, LANES))
        return jnp.swapaxes(a, -3, -2)

    dma = pltpu.SemaphoreType.DMA
    N = len(GROUPS)
    limit = 32 * 1024 * 1024
    buf, peak, where = pl.pallas_call(
        functools.partial(main_kernel, V, S, views),
        out_shape=(
            VMEM((V, nblk, SUB, LANES), f32), VMEM((2 * nblk, LANES), f32), SMEM((SUB, LANES), i32),
        ),
        in_specs=[spec(HBM)] * 10,
        out_specs=(spec(VMEM), spec(VMEM), spec(SMEM)),
        scratch_shapes=[
            SMEM((3, views, 3), f32),
            SMEM((views, 3), f32),
            SMEM((views,), f32),
            VMEM((nblk, LANES), i32),
            VMEM((nblk, 3, LANES), f32),
            VMEM((nblk, 3, LANES), f32),
            VMEM((4 * nblk, LANES), f32),
            VMEM((views, 2 * nblk, LANES), f32),
            VMEM((views * nblk, LANES), i32),
            VMEM((12, nblk, LANES), f32),
            VMEM((SUB, G), f32),
            VMEM((nblk, LANES), i32),
            VMEM((nblk, SUB, LANES), f32),
            VMEM((6 * nblk, SUB * LANES), jnp.bfloat16),
            VMEM((nblk, SUB, LANES), f32),
            VMEM((nblk, SUB, LANES), f32),
            VMEM((SUB, LANES), i32),
            VMEM((1, LANES), i32),
            VMEM((S, LANES), i32),
            VMEM((2 * nblk, LANES), f32),
            VMEM((2 * nblk, LANES), f32),
            VMEM((2 * nblk, LANES), f32),
            VMEM((V // 2 - 1, 2 * nblk, LANES), f32),
            dma((11,)), dma((S,)), dma((S,)), dma((V,)), dma((V,)),
            dma((S,)), dma((S,)), dma((2, N)), dma((2, N)), dma((2, N)), dma((2, N)),
            dma((4, N)), dma((4, N)),
        ],
        compiler_params=pltpu.CompilerParams(
            collective_id=0, has_side_effects=True, vmem_limit_bytes=limit
        ),
        name="main",
    )(*(
        pltpu.with_memory_space_constraint(a, HBM)
        for a in (
            jnp.transpose(rotation, (1, 0, 2)), shift, focal, clone_mask.reshape(nblk, LANES),
            lines(means), lines(scales), lines(quats).reshape(-1, LANES), attrs,
            lines(grad_screen).reshape(views, -1, LANES), lines(visible).reshape(-1, LANES),
        )
    ))
    chunks = 8
    clones, peak, total = pl.pallas_call(
        place_kernel,
        out_shape=(
            jax.ShapeDtypeStruct((rows, G), f32),
            jax.ShapeDtypeStruct((2 * nblk, LANES), f32),
            jax.ShapeDtypeStruct((1,), i32),
        ),
        in_specs=[spec(SMEM), spec(VMEM), spec(VMEM)],
        out_specs=(spec(pl.ANY), spec(pl.ANY), spec(SMEM)),
        scratch_shapes=[VMEM((rows, G), f32), dma((chunks,)), dma],
        compiler_params=pltpu.CompilerParams(vmem_limit_bytes=limit),
        name="place",
    )(where, peak, buf)
    peak = jnp.swapaxes(peak.reshape(nblk, 2, LANES), 0, 1).reshape(2, G)
    return peak, clones, total.reshape(())


def solution(mesh):
    return jax.shard_map(
        functools.partial(body, mesh.shape["view"], mesh.shape["gauss"]),
        mesh=mesh,
        in_specs=(
            P(None, "gauss"),
            P(None, "gauss"),
            P(None, "gauss"),
            P(None, "gauss"),
            P("view", None, "gauss"),
            P("view", "gauss"),
            P("gauss"),
            P("view", None, None),
            P("view", None),
            P("view"),
        ),
        out_specs=(P(None, "gauss"), P(None, "gauss"), P()),
        check_vma=False,
    )
```
